256 devices in a mesh: dap: 16 (over x, z_lo), cplx: 16 (over y, z_hi, core).
Axes of the slice: x: 4, y: 4, z: 8 (z_hi: 2, z_lo: 4; z = z_hi * 4 + z_lo), core: 2. Of those that a mesh axis runs over, the one named last changes fastest.
Arguments:
- pair: bfloat16 [192, 3072, 128], P('dap', 'cplx'), parts along dimension 1, may hold values from -6 to 6
- cotangent: bfloat16 [192, 3072, 128], P('dap', 'cplx'), parts along dimension 1, may hold values from -6 to 6
- residue_mask: int32 [3072], P('cplx'), parts along dimension 0, may hold values 0 or 1
- chain_ids: int32 [3072], P('cplx'), parts along dimension 0, may hold values from 0 to 2, never falling along the last dimension, each value on 1 to 96 neighbouring positions
- chain_embed: float32 [2, 128], replicated, may hold values from -4 to 4
- out_norm_gain: float32 [128], replicated, may hold values from 0.25 to 1.75
- out_proj: bfloat16 [128, 512], replicated, may hold values from -0.5 to 0.5
- out_gate: bfloat16 [128, 128], replicated, may hold values from -0.5 to 0.5
- out_mid_gain: float32 [128], replicated, may hold values from 0.25 to 1.75
- out_final: bfloat16 [128, 128], replicated, may hold values from -0.5 to 0.5
- in_norm_gain: float32 [128], replicated, may hold values from 0.25 to 1.75
- in_proj: bfloat16 [128, 512], replicated, may hold values from -0.5 to 0.5
- in_gate: bfloat16 [128, 128], replicated, may hold values from -0.5 to 0.5
- in_mid_gain: float32 [128], replicated, may hold values from 0.25 to 1.75
- in_final: bfloat16 [128, 128], replicated, may hold values from -0.5 to 0.5
Outputs:
- pair_grad: bfloat16 [192, 3072, 128], P('dap', 'cplx'), parts along dimension 1
- grad_proj: float32 [2048, 512], P('cplx'), parts along dimension 0
- grad_gate: float32 [2048, 128], P('cplx'), parts along dimension 0
- grad_final: float32 [2048, 128], P('cplx'), parts along dimension 0
- grad_norm_gain: float32 [2048], P('cplx'), parts along dimension 0
- grad_mid_gain: float32 [2048], P('cplx'), parts along dimension 0
The draws below stay inside these ranges and needn't reach their ends.
There are 16 independent parts, one for each index of `cplx`. The reference program is written for one: setup_inputs(seed, part) draws one part's arguments, and reference() takes and returns one part's arrays. A program takes and returns all parts, laid end to end along the dimension named above; an argument that names none is the same for every part. Nothing has to cross between parts.
Inputs may be any that keep to these rules, and one draw needn't show every extreme that they name: `chain_ids`: chain numbers never fall along the residues; each chain has at most 96 residues.
All inputs are finite; a program needn't handle non-finite values.
Results may differ from the reference program's by a relative error of at most 0.019.
Values may be sent and summed in bfloat16 or wider, within the bound.
No kernel may reach another device: no remote copies, remote signals or barrier semaphores. Data moves between devices by JAX's collectives and lax.ppermute only.
A program may use at most 128 MiB of HBM per device.

```python
import math
import jax
import jax.numpy as jnp
import numpy as np
from jax import lax

C = 128
HID = 128
N_RES = 192


def plant(result, rng, smallest, high):
    place = [jax.random.randint(jax.random.fold_in(rng, axis), (), 0, length) for axis, length in enumerate(result.shape)]
    widest = result.shape.index(max(result.shape))
    neighbour = place[:widest] + [(place[widest] + 1) % result.shape[widest]] + place[widest + 1:]
    return result.at[tuple(place)].set(smallest).at[tuple(neighbour)].set(high)


def shard_levels(key, extent, cuts, least, high):
    factor_of = 1.0
    for position, blocks in cuts:
        draws = jax.random.uniform(jax.random.fold_in(jax.random.fold_in(key, 6), position), (blocks,), jnp.float32, least / len(cuts), high / len(cuts))
        factor_of = factor_of * jnp.repeat(jnp.exp(draws), extent[position] // blocks).reshape((-1,) + (1,) * (len(extent) - 1 - position))
    return factor_of


def split_up(number_of, total, most, skew):
    loads = [(1 << 20) // math.isqrt(rank ** skew) + 1 for rank in range(2, number_of + 1)]
    surplus, counts = total - most - (number_of - 1), [1] * (number_of - 1)
    while surplus > 0:
        free = [i for i in range(number_of - 1) if counts[i] < most]
        pool, left = sum([loads[i] for i in free]), surplus
        for i in free:
            addition = min(most - counts[i], max(1, left * loads[i] // pool), surplus)
            counts[i] = counts[i] + addition
            surplus = surplus - addition
    return np.array([most] + counts)


def uneven_parts(rng, amount, total, limit, skew):
    if amount == 2:
        one = jax.random.randint(rng, (), max(1, total - limit), min(limit, total - 1) + 1)
        return jnp.stack([one, total - one])
    tallies = jnp.asarray(split_up(amount, total, limit, skew), jnp.int32)
    twos = (amount - 1) // 2
    donor, sink = tallies[1:1 + 2 * twos:2], tallies[2:2 + 2 * twos:2]
    margin = jnp.minimum(donor - 1, limit - sink)
    shifted = jax.random.randint(jax.random.fold_in(rng, 1), (twos,), 0, 1 << 20) % (margin + 1)
    tallies = tallies.at[1:1 + 2 * twos:2].set(donor - shifted).at[2:2 + 2 * twos:2].set(sink + shifted)
    return tallies[jax.random.permutation(jax.random.fold_in(rng, 2), amount)]


def normal_values(stream_key, dims, deviation, most, cuts=(), dtype=jnp.bfloat16):
    drawn = jax.random.normal(stream_key, dims, jnp.float32) * deviation
    if len(cuts) > 0:
        drawn = shard_levels(stream_key, dims, cuts, -0.22, 0.18) * drawn
    return jnp.clip(drawn, min=-most, max=most).astype(dtype)


def setup_inputs(seed: int = 0, part: int = 0) -> dict:
    arg_keys = jax.random.split(jax.random.key(seed), 16)
    part_splits = jax.random.split(jax.random.fold_in(arg_keys[15], part), 16)
    return {
        "pair": normal_values(part_splits[0], (N_RES, N_RES, C), 1.0, 6.0, ((0, 16),)),
        "cotangent": normal_values(part_splits[1], (N_RES, N_RES, C), 1.0, 6.0, ((0, 16),)),
        "residue_mask": plant((jax.random.randint(part_splits[2], (N_RES,), 0, 8) < 7).astype(jnp.int32), jax.random.fold_in(part_splits[2], 1), 0, 1),
        "chain_ids": jnp.searchsorted(jnp.cumsum(uneven_parts(part_splits[3], 3, N_RES, N_RES // 2, 0)), jnp.arange(N_RES), side="right").astype(jnp.int32),
        "chain_embed": normal_values(arg_keys[4], (2, C), 1.0, 4.0, (), jnp.float32),
        "out_norm_gain": jnp.clip(1.0 + 0.15 * jax.random.normal(arg_keys[5], (C,), jnp.float32), 0.25, 1.75),
        "out_proj": normal_values(arg_keys[6], (C, 4 * HID), C ** -0.5, 0.5),
        "out_gate": normal_values(arg_keys[7], (C, C), C ** -0.5, 0.5),
        "out_mid_gain": jnp.clip(1.0 + 0.15 * jax.random.normal(arg_keys[8], (HID,), jnp.float32), 0.25, 1.75),
        "out_final": normal_values(arg_keys[9], (HID, C), HID ** -0.5, 0.5),
        "in_norm_gain": jnp.clip(1.0 + 0.15 * jax.random.normal(arg_keys[10], (C,), jnp.float32), 0.25, 1.75),
        "in_proj": normal_values(arg_keys[11], (C, 4 * HID), C ** -0.5, 0.5),
        "in_gate": normal_values(arg_keys[12], (C, C), C ** -0.5, 0.5),
        "in_mid_gain": jnp.clip(1.0 + 0.15 * jax.random.normal(arg_keys[13], (HID,), jnp.float32), 0.25, 1.75),
        "in_final": normal_values(arg_keys[14], (HID, C), HID ** -0.5, 0.5),
    }


def layer_norm(values_in, gain):
    average = lax.optimization_barrier(jnp.mean(values_in, axis=-1, keepdims=True))
    centred = values_in - average
    variance = lax.optimization_barrier(jnp.mean(centred * centred, axis=-1, keepdims=True))
    return centred * jax.lax.rsqrt(variance + 1e-05) * gain

def gated_pair(projected, pair_mask, hidden_width):
    masked = pair_mask[..., None]
    left_act = masked * jax.nn.sigmoid(projected[..., :hidden_width]) * projected[..., hidden_width:2 * hidden_width]
    right_act = masked * jax.nn.sigmoid(projected[..., 2 * hidden_width:3 * hidden_width]) * projected[..., 3 * hidden_width:]
    return (left_act, right_act)

def reference(pair, cotangent, residue_mask, chain_ids, chain_embed, out_norm_gain, out_proj, out_gate, out_mid_gain, out_final, in_norm_gain, in_proj, in_gate, in_mid_gain, in_final):
    f32 = jnp.float32
    bf16 = jnp.bfloat16
    hidden_width = out_final.shape[0]
    res_count = pair.shape[0]
    inv_count = 1.0 / res_count
    pair_mask = (residue_mask[:, None] * residue_mask[None, :]).astype(f32)
    same_chain = chain_ids[:, None] == chain_ids[None, :]
    start = pair.astype(f32) + jnp.where(same_chain[..., None], chain_embed[1], chain_embed[0])
    out_normed = layer_norm(start, out_norm_gain).astype(bf16)
    projected = jnp.dot(out_normed, out_proj, preferred_element_type=f32)
    left_act, right_act = gated_pair(projected, pair_mask, hidden_width)
    left_b = left_act.astype(bf16)
    right_b = right_act.astype(bf16)
    x_out = jnp.einsum('ikc,jkc->ijc', left_b.astype(f32), right_b.astype(f32))
    y_out = layer_norm(x_out, out_mid_gain).astype(bf16)
    update = jax.nn.sigmoid(jnp.dot(out_normed, out_gate, preferred_element_type=f32)) * jnp.dot(y_out, out_final, preferred_element_type=f32)
    pair_mid = (start + update).astype(bf16)
    mid_f32 = pair_mid.astype(f32)
    normed_f32, norm_back = jax.vjp(layer_norm, mid_f32, in_norm_gain)
    in_normed = normed_f32.astype(bf16)
    proj_in = jnp.dot(in_normed, in_proj, preferred_element_type=f32)
    (left_in, right_in), glu_back = jax.vjp(lambda proj_val: gated_pair(proj_val, pair_mask, hidden_width), proj_in)
    left_ib = left_in.astype(bf16)
    right_ib = right_in.astype(bf16)
    x_in = jnp.einsum('kic,kjc->ijc', left_ib.astype(f32), right_ib.astype(f32))
    y_f32, mid_back = jax.vjp(layer_norm, x_in, in_mid_gain)
    y_in = y_f32.astype(bf16)
    logit = jnp.dot(in_normed, in_gate, preferred_element_type=f32)
    value = jnp.dot(y_in, in_final, preferred_element_type=f32)
    sigma = jax.nn.sigmoid(logit)
    upstream = cotangent.astype(f32)
    grad_value = (upstream * sigma).astype(bf16)
    grad_logit = (upstream * value * sigma * (1.0 - sigma)).astype(bf16)
    grad_final = jnp.einsum('ijc,ijd->cd', y_in.astype(f32), grad_value.astype(f32)) * inv_count
    grad_gate = jnp.einsum('ijc,ijd->cd', in_normed.astype(f32), grad_logit.astype(f32)) * inv_count
    grad_y = jnp.dot(grad_value, in_final.T, preferred_element_type=f32)
    grad_x, grad_mid = mid_back(grad_y)
    grad_x_b = grad_x.astype(bf16).astype(f32)
    grad_a = jnp.einsum('kjc,ijc->kic', right_ib.astype(f32), grad_x_b)
    grad_b = jnp.einsum('kic,ijc->kjc', left_ib.astype(f32), grad_x_b)
    grad_p = glu_back((grad_a, grad_b))[0].astype(bf16)
    grad_proj = jnp.einsum('ijc,ijd->cd', in_normed.astype(f32), grad_p.astype(f32)) * inv_count
    grad_normed = jnp.dot(grad_p, in_proj.T, preferred_element_type=f32) + jnp.dot(grad_logit, in_gate.T, preferred_element_type=f32)
    grad_z, grad_norm = norm_back(grad_normed)
    pair_grad = (upstream + grad_z).astype(bf16)
    return (pair_grad, grad_proj, grad_gate, grad_final, grad_norm * inv_count, grad_mid * inv_count)
```

```python
import jax
import jax.numpy as jnp
from jax import lax
from jax.experimental import pallas as pl
from jax.experimental.pallas import tpu as pltpu
from jax.sharding import PartitionSpec as P

F32 = jnp.float32
BF16 = jnp.bfloat16
AXIS = "dap"
DEVS = 16
ROWS = 12
RES = 192
CH = 128
CPD = CH // DEVS
POS = ROWS * RES
TILE = 2 * RES
STEPS = POS // TILE
LANES = 128
LTILES = POS // LANES
GCOLS = 7 * CH
EPS = 1e-05


def dot_nn(a, b):
    return lax.dot_general(a, b, (((1,), (0,)), ((), ())), preferred_element_type=F32)


def dot_nt(a, b):
    return lax.dot_general(a, b, (((1,), (1,)), ((), ())), preferred_element_type=F32)


def dot_tn(a, b):
    return lax.dot_general(a, b, (((0,), (0,)), ((), ())), preferred_element_type=F32)


def column(row):
    block = jnp.transpose(jnp.broadcast_to(row, (CH, LANES)))
    return jnp.concatenate([block] * (TILE // LANES), axis=1)


def sigmoid(v):
    return 1.0 / (1.0 + jnp.exp(-v))


def stats(v):
    centred = v - jnp.mean(v, axis=0, keepdims=True)
    variance = jnp.mean(centred * centred, axis=0, keepdims=True)
    return centred, lax.rsqrt(variance + EPS)


def norm_grad(hat, rstd, gain, grad):
    h = grad * gain
    return rstd * (
        h - jnp.mean(h, axis=0, keepdims=True) - hat * jnp.mean(h * hat, axis=0, keepdims=True)
    )


def tile_rows(first_ref, table_ref, step):
    base = first_ref[0] + 2 * step
    lane = lax.broadcasted_iota(jnp.int32, (1, TILE), 1)
    return jnp.where(lane < RES, table_ref[base], table_ref[base + 1])


def tile_mask(first_ref, mask_ref, lanes_ref, step):
    return (tile_rows(first_ref, mask_ref, step) * lanes_ref[0:1, :]).astype(F32)


def interleave(left, right):
    n = left.shape[1]
    both = jnp.stack([left.reshape(DEVS, CPD, n), right.reshape(DEVS, CPD, n)], axis=1)
    return both.reshape(DEVS, 2 * CPD, n)


def lane_sums(v):
    return sum(v[:, i * LANES : (i + 1) * LANES] for i in range(v.shape[1] // LANES))


def first_kernel(first, mask, chain, lanes, pair, embed, gain, proj, gate, send, start, gated):
    step = pl.program_id(0)
    pm = tile_mask(first, mask, lanes, step)
    same = tile_rows(first, chain, step) == lanes[1:2, :]
    values = jnp.transpose(pair[...].astype(F32).reshape(TILE, CH))
    values = values + jnp.where(same, column(embed[1:2, :]), column(embed[0:1, :]))
    start[...] = values
    centred, rstd = stats(values)
    normed = (centred * rstd * column(gain[...])).astype(BF16)
    p = dot_tn(proj[...], normed)
    left = pm * sigmoid(p[:CH]) * p[CH : 2 * CH]
    right = pm * sigmoid(p[2 * CH : 3 * CH]) * p[3 * CH :]
    send[...] = interleave(left, right).astype(BF16)
    gated[...] = sigmoid(dot_tn(gate[...], normed))


def middle_kernel(
    first, mask, lanes, xs, start, gated, mid_gain, final, gain, proj, send, pair_mid, in_normed
):
    step = pl.program_id(0)
    pm = tile_mask(first, mask, lanes, step)
    centred, rstd = stats(xs[...].astype(F32).reshape(CH, TILE))
    y = (centred * rstd * column(mid_gain[...])).astype(BF16)
    mid = (start[...] + gated[...] * dot_tn(final[...], y)).astype(BF16)
    pair_mid[...] = mid
    centred, rstd = stats(mid.astype(F32))
    normed = (centred * rstd * column(gain[...])).astype(BF16)
    in_normed[...] = normed
    p = dot_tn(proj[...], normed)
    left = pm * sigmoid(p[:CH]) * p[CH : 2 * CH]
    right = pm * sigmoid(p[2 * CH : 3 * CH]) * p[3 * CH :]
    send[...] = interleave(left, right).astype(BF16)


def turn_kernel(xs, cot, in_normed, mid_gain, gate, final, send, grad_logit, sums):
    step = pl.program_id(0)
    gain = column(mid_gain[...])
    centred, rstd = stats(xs[...].astype(F32).reshape(CH, TILE))
    hat = centred * rstd
    y = (hat * gain).astype(BF16)
    normed = in_normed[...]
    sigma = sigmoid(dot_tn(gate[...], normed))
    value = dot_tn(final[...], y)
    upstream = jnp.transpose(cot[...].astype(F32).reshape(TILE, CH))
    grad_value = (upstream * sigma).astype(BF16)
    grad_lg = (upstream * value * sigma * (1.0 - sigma)).astype(BF16)
    grad_logit[...] = grad_lg
    grad_y = dot_nn(final[...], grad_value)
    send[...] = norm_grad(hat, rstd, gain, grad_y).astype(BF16).reshape(DEVS, CPD, TILE)

    @pl.when(step == 0)
    def _():
        sums[...] = jnp.zeros_like(sums)

    sums[:, :CH] += dot_nt(normed, grad_lg)
    sums[:, CH : 2 * CH] += dot_nt(y, grad_value)
    sums[:, 2 * CH :] += lane_sums(grad_y * hat)


def last_kernel(
    first, mask, lanes, gs, cot, in_normed, pair_mid, grad_logit, gain_row, proj, gate, sums,
    pair_grad, packed, acc_proj, acc_gain,
):
    step = pl.program_id(0)
    pm = tile_mask(first, mask, lanes, step)
    normed = in_normed[...]
    p = dot_tn(proj[...], normed)
    grads = gs[...].astype(F32).reshape(DEVS, 2, CPD, TILE)
    parts = []
    for side in range(2):
        grad = pm * grads[:, side].reshape(CH, TILE)
        sig = sigmoid(p[2 * side * CH : (2 * side + 1) * CH])
        val = p[(2 * side + 1) * CH : (2 * side + 2) * CH]
        parts.append((grad * val * sig * (1.0 - sig)).astype(BF16))
        parts.append((grad * sig).astype(BF16))
    grad_p = jnp.concatenate(parts, axis=0)
    grad_normed = dot_nn(proj[...], grad_p) + dot_nn(gate[...], grad_logit[...])
    centred, rstd = stats(pair_mid[...].astype(F32))
    hat = centred * rstd
    grad_z = norm_grad(hat, rstd, column(gain_row[...]), grad_normed)
    out = cot[...].astype(F32).reshape(TILE, CH) + jnp.transpose(grad_z)
    pair_grad[...] = out.astype(BF16).reshape(2, RES, CH)

    @pl.when(step == 0)
    def _():
        acc_proj[...] = jnp.zeros_like(acc_proj)
        acc_gain[...] = jnp.zeros_like(acc_gain)

    acc_proj[...] += dot_nt(normed, grad_p)
    acc_gain[...] += lane_sums(grad_normed * hat)

    @pl.when(step == STEPS - 1)
    def _():
        lane = lax.broadcasted_iota(jnp.int32, (CH, LANES), 1)
        norm_sum = jnp.sum(acc_gain[...], axis=1, keepdims=True)
        mid_sum = jnp.sum(sums[:, 2 * CH :], axis=1, keepdims=True)
        gains = jnp.where(lane == 0, norm_sum, jnp.where(lane == 1, mid_sum, 0.0))
        full = jnp.concatenate([acc_proj[...], sums[:, : 2 * CH], gains], axis=1)
        packed[...] = (full * (1.0 / RES)).astype(BF16).reshape(DEVS, CPD, GCOLS)


def add_kernel(parts, out):
    total = jnp.sum(parts[...].astype(F32), axis=0).astype(BF16)
    out[...] = jnp.broadcast_to(total[None], out.shape)


def unpack_kernel(parts, proj, gate, final, gains):
    full = parts[...].astype(F32).reshape(CH, GCOLS)
    proj[...] = full[:, : 4 * CH]
    gate[...] = full[:, 4 * CH : 5 * CH]
    final[...] = full[:, 5 * CH : 6 * CH]
    gains[...] = jnp.transpose(full[:, 6 * CH :])[:8]


def unfold(recv, flat, width):
    rows = DEVS * width
    for t in range(LTILES):
        block = recv[:, :, t * LANES : (t + 1) * LANES].astype(F32)
        flat[t * rows : (t + 1) * rows, :] = block.reshape(rows, LANES)


def fold(flat, send, width):
    rows = DEVS * width
    for t in range(LTILES):
        block = flat[t * rows : (t + 1) * rows, :].reshape(DEVS, width, LANES)
        send[:, :, t * LANES : (t + 1) * LANES] = block.astype(BF16)


def low_half():
    return lax.broadcasted_iota(jnp.int32, (DEVS, LANES), 1) < LANES // 2


def gather_matrix(flat, width, c, mat):
    rows = DEVS * width
    low = low_half()
    for q in range(STEPS):
        t0, t1, t2 = (
            flat[pl.ds((3 * q + h) * rows + c, DEVS, stride=width), :] for h in range(3)
        )
        r1 = pltpu.roll(t1, LANES // 2, axis=1)
        r2 = pltpu.roll(t2, LANES // 2, axis=1)
        mat[pl.ds(2 * q, DEVS, stride=ROWS), :] = t0
        mat[pl.ds(RES + 2 * q, DEVS, stride=ROWS), :] = t1
        mat[pl.ds(2 * q + 1, DEVS, stride=ROWS), :] = jnp.where(low, r1, r2)
        mat[pl.ds(RES + 2 * q + 1, DEVS, stride=ROWS), :] = r2
    full = jnp.concatenate([mat[:RES, :], mat[RES:, :]], axis=1)
    return full[:, :RES].astype(BF16)


def scatter_matrix(value, mat, flat, width, c):
    rows = DEVS * width
    low = low_half()
    mat[:RES, :] = value[:, :LANES]
    mat[RES:, : RES - LANES] = value[:, LANES:]
    for q in range(STEPS):
        e0 = mat[pl.ds(2 * q, DEVS, stride=ROWS), :]
        e1 = mat[pl.ds(RES + 2 * q, DEVS, stride=ROWS), :]
        o0 = pltpu.roll(mat[pl.ds(2 * q + 1, DEVS, stride=ROWS), :], LANES // 2, axis=1)
        o1 = pltpu.roll(mat[pl.ds(RES + 2 * q + 1, DEVS, stride=ROWS), :], LANES // 2, axis=1)
        tiles = (e0, jnp.where(low, e1, o0), jnp.where(low, o0, o1))
        for h in range(3):
            flat[pl.ds((3 * q + h) * rows + c, DEVS, stride=width), :] = tiles[h]


def outgoing_kernel(recv, send, flat, mat_a, mat_b, out):
    unfold(recv, flat, 2 * CPD)
    for c in range(CPD):
        a = gather_matrix(flat, 2 * CPD, c, mat_a)
        b = gather_matrix(flat, 2 * CPD, CPD + c, mat_b)
        scatter_matrix(dot_nt(a, b), mat_a, out, CPD, c)
    fold(out, send, CPD)


def incoming_kernel(recv, send, sides, flat, mat_a, mat_b, out):
    unfold(recv, flat, 2 * CPD)
    for c in range(CPD):
        a = gather_matrix(flat, 2 * CPD, c, mat_a)
        b = gather_matrix(flat, 2 * CPD, CPD + c, mat_b)
        sides[c] = a
        sides[CPD + c] = b
        scatter_matrix(dot_tn(a, b), mat_a, out, CPD, c)
    fold(out, send, CPD)


def backward_kernel(recv, sides, send, flat, mat_a, mat_b, out):
    unfold(recv, flat, CPD)
    for c in range(CPD):
        g = gather_matrix(flat, CPD, c, mat_a)
        scatter_matrix(dot_nt(sides[CPD + c], g), mat_a, out, 2 * CPD, c)
        scatter_matrix(dot_nn(sides[c], g), mat_b, out, 2 * CPD, CPD + c)
    fold(out, send, 2 * CPD)


def product(kernel, args, out_shape, width_in, width_out, name):
    return pl.pallas_call(
        kernel,
        out_shape=out_shape,
        scratch_shapes=[
            pltpu.VMEM((LTILES * DEVS * width_in, LANES), F32),
            pltpu.VMEM((2 * RES, LANES), F32),
            pltpu.VMEM((2 * RES, LANES), F32),
            pltpu.VMEM((LTILES * DEVS * width_out, LANES), F32),
        ],
        name=name,
    )(*args)


SMEM = pl.BlockSpec(memory_space=pltpu.SMEM)


def whole(shape):
    return pl.BlockSpec(shape, lambda i: (0,) * len(shape))


def tiled(*lead):
    return pl.BlockSpec((*lead, TILE), lambda i: (0,) * len(lead) + (i,))


ROW_BLOCK = pl.BlockSpec((2, RES, CH), lambda i: (i, 0, 0))
GAIN = whole((1, CH))
LANE_INFO = whole((2, TILE))


def over_tiles(kernel, args, in_specs, out_specs, out_shape, name, scratch=()):
    return pl.pallas_call(
        kernel,
        grid=(STEPS,),
        in_specs=in_specs,
        out_specs=out_specs,
        out_shape=out_shape,
        scratch_shapes=scratch,
        name=name,
    )(*args)


def shaped(shape, dtype=BF16):
    return jax.ShapeDtypeStruct(shape, dtype)


def exchange(v):
    return lax.all_to_all(v, AXIS, 0, 0)


def shards(
    pair,
    cotangent,
    residue_mask,
    chain_ids,
    chain_embed,
    out_norm_gain,
    out_proj,
    out_gate,
    out_mid_gain,
    out_final,
    in_norm_gain,
    in_proj,
    in_gate,
    in_mid_gain,
    in_final,
):
    first = (lax.axis_index(AXIS) * ROWS).astype(jnp.int32).reshape(1)
    info = jnp.stack([residue_mask, chain_ids])
    info = jnp.concatenate([info, info], axis=1)
    gains = [g.reshape(1, CH) for g in (out_norm_gain, out_mid_gain, in_norm_gain, in_mid_gain)]
    square = whole((CH, CH))
    wide = whole((CH, 4 * CH))
    pair_send = shaped((DEVS, 2 * CPD, POS))
    one_send = shaped((DEVS, CPD, POS))

    send, start, gated = over_tiles(
        first_kernel,
        (first, residue_mask, chain_ids, info, pair, chain_embed, gains[0], out_proj, out_gate),
        [SMEM, SMEM, SMEM, LANE_INFO, ROW_BLOCK, whole((2, CH)), GAIN, wide, square],
        [tiled(DEVS, 2 * CPD), tiled(CH), tiled(CH)],
        [pair_send, shaped((CH, POS), F32), shaped((CH, POS), F32)],
        "first",
    )
    x_out = product(outgoing_kernel, (exchange(send),), one_send, 2 * CPD, CPD, "outgoing")
    send, pair_mid, in_normed = over_tiles(
        middle_kernel,
        (first, residue_mask, info, exchange(x_out), start, gated, gains[1], out_final, gains[2], in_proj),
        [SMEM, SMEM, LANE_INFO, tiled(DEVS, CPD), tiled(CH), tiled(CH), GAIN, square, GAIN, wide],
        [tiled(DEVS, 2 * CPD), tiled(CH), tiled(CH)],
        [pair_send, shaped((CH, POS)), shaped((CH, POS))],
        "middle",
    )
    x_in, sides = product(
        incoming_kernel,
        (exchange(send),),
        [one_send, shaped((2 * CPD, RES, RES))],
        2 * CPD,
        CPD,
        "incoming",
    )
    send, grad_logit, sums = over_tiles(
        turn_kernel,
        (exchange(x_in), cotangent, in_normed, gains[3], in_gate, in_final),
        [tiled(DEVS, CPD), ROW_BLOCK, tiled(CH), GAIN, square, square],
        [tiled(DEVS, CPD), tiled(CH), whole((CH, 3 * CH))],
        [one_send, shaped((CH, POS)), shaped((CH, 3 * CH), F32)],
        "turn",
    )
    grads = product(backward_kernel, (exchange(send), sides), pair_send, CPD, 2 * CPD, "backward")
    pair_grad, packed = over_tiles(
        last_kernel,
        (first, residue_mask, info, exchange(grads), cotangent, in_normed, pair_mid, grad_logit,
         gains[2], in_proj, in_gate, sums),
        [SMEM, SMEM, LANE_INFO, tiled(DEVS, 2 * CPD), ROW_BLOCK, tiled(CH), tiled(CH), tiled(CH),
         GAIN, wide, square, whole((CH, 3 * CH))],
        [ROW_BLOCK, whole((DEVS, CPD, GCOLS))],
        [shaped((ROWS, RES, CH)), shaped((DEVS, CPD, GCOLS))],
        "last",
        [pltpu.VMEM((CH, 4 * CH), F32), pltpu.VMEM((CH, LANES), F32)],
    )
    total = pl.pallas_call(add_kernel, out_shape=shaped((DEVS, CPD, GCOLS)), name="add")(
        exchange(packed)
    )
    grad_proj, grad_gate, grad_final, grad_gains = pl.pallas_call(
        unpack_kernel,
        out_shape=[shaped((CH, 4 * CH), F32), shaped((CH, CH), F32), shaped((CH, CH), F32), shaped((8, CH), F32)],
        name="unpack",
    )(exchange(total))
    return pair_grad, grad_proj, grad_gate, grad_final, grad_gains[0], grad_gains[1]


def solution(mesh):
    rows = P("dap", "cplx", None)
    return jax.shard_map(
        shards,
        mesh=mesh,
        in_specs=(rows, rows, P("cplx"), P("cplx")) + (P(),) * 11,
        out_specs=(
            rows,
            P("cplx", None),
            P("cplx", None),
            P("cplx", None),
            P("cplx"),
            P("cplx"),
        ),
        check_vma=False,
    )
```

```python
import jax
import jax.numpy as jnp
from jax import lax
from jax.experimental import pallas as pl
from jax.experimental.pallas import tpu as pltpu
from jax.sharding import PartitionSpec as P

F32 = jnp.float32
BF16 = jnp.bfloat16
AXIS = "dap"
DEVS = 16
ROWS = 12
RES = 192
CH = 128
CPD = CH // DEVS
POS = ROWS * RES
TROWS = 6
TILE = TROWS * RES
STEPS = POS // TILE
LANES = 128
LTILES = POS // LANES
GCOLS = 6 * CH
EPS = 1e-05


def dot_nn(a, b):
    return lax.dot_general(a, b, (((1,), (0,)), ((), ())), preferred_element_type=F32)


def dot_nt(a, b):
    return lax.dot_general(a, b, (((1,), (1,)), ((), ())), preferred_element_type=F32)


def dot_tn(a, b):
    return lax.dot_general(a, b, (((0,), (0,)), ((), ())), preferred_element_type=F32)


def column(row):
    block = jnp.transpose(jnp.broadcast_to(row, (CH, LANES)))
    return jnp.concatenate([block] * (TILE // LANES), axis=1)


def sigmoid(v):
    return 0.5 + 0.5 * jnp.tanh(0.5 * v)


def stats(v):
    centred = v - jnp.mean(v, axis=0, keepdims=True)
    variance = jnp.mean(centred * centred, axis=0, keepdims=True)
    return centred, lax.rsqrt(variance + EPS)


def norm_grad(hat, rstd, h):
    return rstd * (
        h - jnp.mean(h, axis=0, keepdims=True) - hat * jnp.mean(h * hat, axis=0, keepdims=True)
    )


def window(step):
    return pl.ds(pl.multiple_of(step * TILE, TILE), TILE)


def tile_rows(first_ref, table_ref, step):
    base = first_ref[0] + TROWS * step
    lane = lax.broadcasted_iota(jnp.int32, (1, TILE), 1)
    out = jnp.full((1, TILE), table_ref[base], jnp.int32)
    for r in range(1, TROWS):
        out = jnp.where(lane < r * RES, out, table_ref[base + r])
    return out


def along_lanes(row_ref, wide_ref):
    wide_ref[...] = jnp.zeros_like(wide_ref)
    wide_ref[:1, :RES] = row_ref[...]
    row = wide_ref[...]
    lane = lax.broadcasted_iota(jnp.int32, row.shape, 1)
    double = jnp.where(lane < RES, row, pltpu.roll(row, RES, axis=1))[0:1]
    return jnp.concatenate([double] * (TROWS // 2), axis=1)


def tile_mask(first_ref, mask_ref, row_ref, wide_ref, step):
    return (tile_rows(first_ref, mask_ref, step) * along_lanes(row_ref, wide_ref)).astype(F32)


def interleave(left, right):
    n = left.shape[1]
    both = jnp.stack([left.reshape(DEVS, CPD, n), right.reshape(DEVS, CPD, n)], axis=1)
    return both.reshape(DEVS, 2 * CPD, n)


def lane_sums(v):
    return sum(v[:, i * LANES : (i + 1) * LANES] for i in range(v.shape[1] // LANES))


def turned(block):
    return jnp.transpose(block.astype(F32).reshape(TILE, CH))


def gated_pair(pm, p):
    left = pm * sigmoid(p[:CH]) * p[CH : 2 * CH]
    right = pm * sigmoid(p[2 * CH : 3 * CH]) * p[3 * CH :]
    return interleave(left, right).astype(BF16)


def first_kernel(
    first, mask, chain, mask_row, chain_row, pair, embed, gain, proj, send, start, normed_out, wide
):
    step = pl.program_id(0)
    pm = tile_mask(first, mask, mask_row, wide, step)
    same = tile_rows(first, chain, step) == along_lanes(chain_row, wide)
    values = turned(pair[...])
    values = values + jnp.where(same, column(embed[1:2, :]), column(embed[0:1, :]))
    start[...] = values
    centred, rstd = stats(values)
    normed = (centred * rstd * column(gain[...])).astype(BF16)
    normed_out[...] = normed
    send[:, :, window(step)] = gated_pair(pm, dot_tn(proj[...], normed))


def gate_kernel(normed, gate, gated):
    gated[...] = sigmoid(dot_tn(gate[...], normed[...]))


def middle_kernel(
    first, mask, mask_row, xs, start, gated, mid_gain, final, gain, proj, send, pair_mid, in_normed,
    wide,
):
    step = pl.program_id(0)
    pm = tile_mask(first, mask, mask_row, wide, step)
    centred, rstd = stats(xs[:, :, window(step)].astype(F32).reshape(CH, TILE))
    y = (centred * rstd * column(mid_gain[...])).astype(BF16)
    mid = (start[...] + gated[...] * dot_tn(final[...], y)).astype(BF16)
    pair_mid[...] = mid
    centred, rstd = stats(mid.astype(F32))
    normed = (centred * rstd * column(gain[...])).astype(BF16)
    in_normed[...] = normed
    send[:, :, window(step)] = gated_pair(pm, dot_tn(proj[...], normed))


def ahead_kernel(first, mask, mask_row, cot, in_normed, gain, gate, final, proj,
                 grad_value, grad_h, factor, factors, wide):
    step = pl.program_id(0)
    pm = tile_mask(first, mask, mask_row, wide, step)
    normed = in_normed[...]
    sigma = sigmoid(dot_tn(gate[...], normed))
    upstream = turned(cot[...])
    scaled = upstream * sigma
    rounded = scaled.astype(BF16)
    grad_value[...] = rounded
    factor[...] = scaled * (1.0 - sigma)
    grad_h[...] = dot_nn(final[...], rounded) * column(gain[...])
    p = dot_tn(proj[...], normed)
    for side in range(2):
        low = 2 * side * CH
        raw = sigmoid(p[low : low + CH])
        sig = pm * raw
        factors[low : low + CH, :] = (sig * p[low + CH : low + 2 * CH] * (1.0 - raw)).astype(BF16)
        factors[low + CH : low + 2 * CH, :] = sig.astype(BF16)


def turn_kernel(xs, grad_h, send):
    step = pl.program_id(0)
    centred, rstd = stats(xs[:, :, window(step)].astype(F32).reshape(CH, TILE))
    grad_x = norm_grad(centred * rstd, rstd, grad_h[...])
    send[:, :, window(step)] = grad_x.astype(BF16).reshape(DEVS, CPD, TILE)


def after_kernel(xs, in_normed, grad_value, factor, gain, final, gate, sums, from_gate):
    step = pl.program_id(0)
    centred, rstd = stats(xs[:, :, window(step)].astype(F32).reshape(CH, TILE))
    hat = centred * rstd
    y = (hat * column(gain[...])).astype(BF16)
    normed = in_normed[...]
    rounded = grad_value[...]
    grad_logit = (factor[...] * dot_tn(final[...], y)).astype(BF16)
    grad_y = dot_nn(final[...], rounded)
    from_gate[...] = dot_nn(gate[...], grad_logit)

    @pl.when(step == 0)
    def _():
        sums[...] = jnp.zeros_like(sums)

    sums[:, :CH] += dot_nt(normed, grad_logit)
    sums[:, CH : 2 * CH] += dot_nt(y, rounded)
    sums[:, 2 * CH :] += lane_sums(grad_y * hat)


def last_kernel(gs, in_normed, factors, sums, grad_p, packed, acc_proj):
    step = pl.program_id(0)
    grads = gs[:, :, window(step)].astype(F32).reshape(DEVS, 2, CPD, TILE)
    for side in range(2):
        grad = grads[:, side].reshape(CH, TILE)
        for part in range(2):
            low = (2 * side + part) * CH
            grad_p[low : low + CH, :] = (grad * factors[low : low + CH, :].astype(F32)).astype(BF16)

    @pl.when(step == 0)
    def _():
        acc_proj[...] = jnp.zeros_like(acc_proj)

    acc_proj[...] += dot_nt(in_normed[...], grad_p[...])

    @pl.when(step == STEPS - 1)
    def _():
        full = jnp.concatenate([acc_proj[...], sums[:, : 2 * CH]], axis=1)
        packed[...] = (full * (1.0 / RES)).astype(BF16).reshape(DEVS, CPD, GCOLS)


def norm_kernel(cot, pair_mid, grad_p, from_gate, gain, proj, sums, pair_grad, gains, acc):
    step = pl.program_id(0)
    grad_normed = dot_nn(proj[...], grad_p[...]) + from_gate[...]
    centred, rstd = stats(pair_mid[...].astype(F32))
    hat = centred * rstd
    grad_z = norm_grad(hat, rstd, grad_normed * column(gain[...]))
    out = cot[...].astype(F32).reshape(TILE, CH) + jnp.transpose(grad_z)
    pair_grad[...] = out.astype(BF16).reshape(TROWS, RES, CH)

    @pl.when(step == 0)
    def _():
        acc[...] = jnp.zeros_like(acc)

    acc[...] += lane_sums(grad_normed * hat)

    @pl.when(step == STEPS - 1)
    def _():
        norm_row = jnp.sum(jnp.transpose(acc[...]), axis=0, keepdims=True)
        mid_row = jnp.sum(jnp.transpose(sums[:, 2 * CH :]), axis=0, keepdims=True)
        index = lax.broadcasted_iota(jnp.int32, (CPD, CH), 0)
        rows = jnp.where(index == 0, norm_row, jnp.where(index == 1, mid_row, 0.0))
        gains[...] = rows * (1.0 / RES)


def add_kernel(parts, gains, out):
    total = jnp.sum(parts[...].astype(F32), axis=0)
    total = jnp.concatenate([total, gains[...]], axis=1).astype(BF16)
    out[...] = jnp.broadcast_to(total[None], out.shape)


def unpack_kernel(parts, proj, gate, final, norm_gain, mid_gain):
    full = parts[:, :, :GCOLS].astype(F32).reshape(CH, GCOLS)
    proj[...] = full[:, : 4 * CH]
    gate[...] = full[:, 4 * CH : 5 * CH]
    final[...] = full[:, 5 * CH :]
    gains = jnp.sum(parts[:, :, GCOLS:].astype(F32), axis=0)
    norm_gain[...] = gains[0:1]
    mid_gain[...] = gains[1:2]


def unfold(recv, flat, width):
    rows = DEVS * width
    for t in range(LTILES):
        block = recv[:, :, t * LANES : (t + 1) * LANES].astype(F32)
        flat[t * rows : (t + 1) * rows, :] = block.reshape(rows, LANES)


def fold(flat, send, width):
    rows = DEVS * width
    for t in range(LTILES):
        block = flat[t * rows : (t + 1) * rows, :].reshape(DEVS, width, LANES)
        send[:, :, t * LANES : (t + 1) * LANES] = block.astype(BF16)


def low_half():
    return lax.broadcasted_iota(jnp.int32, (DEVS, LANES), 1) < LANES // 2


def gather_matrix(flat, width, c, mat):
    rows = DEVS * width
    low = low_half()
    for q in range(ROWS // 2):
        t0, t1, t2 = (
            flat[pl.ds((3 * q + h) * rows + c, DEVS, stride=width), :] for h in range(3)
        )
        r1 = pltpu.roll(t1, LANES // 2, axis=1)
        r2 = pltpu.roll(t2, LANES // 2, axis=1)
        mat[pl.ds(2 * q, DEVS, stride=ROWS), :] = t0
        mat[pl.ds(RES + 2 * q, DEVS, stride=ROWS), :] = t1
        mat[pl.ds(2 * q + 1, DEVS, stride=ROWS), :] = jnp.where(low, r1, r2)
        mat[pl.ds(RES + 2 * q + 1, DEVS, stride=ROWS), :] = r2
    full = jnp.concatenate([mat[:RES, :], mat[RES:, :]], axis=1)
    return full[:, :RES].astype(BF16)


def scatter_matrix(value, mat, flat, width, c):
    rows = DEVS * width
    low = low_half()
    mat[:RES, :] = value[:, :LANES]
    mat[RES:, : RES - LANES] = value[:, LANES:]
    for q in range(ROWS // 2):
        e0 = mat[pl.ds(2 * q, DEVS, stride=ROWS), :]
        e1 = mat[pl.ds(RES + 2 * q, DEVS, stride=ROWS), :]
        o0 = pltpu.roll(mat[pl.ds(2 * q + 1, DEVS, stride=ROWS), :], LANES // 2, axis=1)
        o1 = pltpu.roll(mat[pl.ds(RES + 2 * q + 1, DEVS, stride=ROWS), :], LANES // 2, axis=1)
        tiles = (e0, jnp.where(low, e1, o0), jnp.where(low, o0, o1))
        for h in range(3):
            flat[pl.ds((3 * q + h) * rows + c, DEVS, stride=width), :] = tiles[h]


def outgoing_kernel(recv, send, flat, mats_a, mats_b, out):
    unfold(recv, flat, 2 * CPD)
    for c in range(CPD):
        a = gather_matrix(flat, 2 * CPD, c, mats_a.at[c])
        b = gather_matrix(flat, 2 * CPD, CPD + c, mats_b.at[c])
        scatter_matrix(dot_nt(a, b), mats_a.at[c], out, CPD, c)
    fold(out, send, CPD)


def incoming_kernel(recv, send, sides, flat, mats_a, mats_b, out):
    unfold(recv, flat, 2 * CPD)
    for c in range(CPD):
        a = gather_matrix(flat, 2 * CPD, c, mats_a.at[c])
        b = gather_matrix(flat, 2 * CPD, CPD + c, mats_b.at[c])
        sides[c] = a
        sides[CPD + c] = b
        scatter_matrix(dot_tn(a, b), mats_a.at[c], out, CPD, c)
    fold(out, send, CPD)


def backward_kernel(recv, sides, send, flat, mats_a, mats_b, out):
    unfold(recv, flat, CPD)
    for c in range(CPD):
        g = gather_matrix(flat, CPD, c, mats_a.at[c])
        scatter_matrix(dot_nt(sides[CPD + c], g), mats_a.at[c], out, 2 * CPD, c)
        scatter_matrix(dot_nn(sides[c], g), mats_b.at[c], out, 2 * CPD, CPD + c)
    fold(out, send, 2 * CPD)


def product(kernel, args, out_shape, width_in, width_out, name):
    return pl.pallas_call(
        kernel,
        out_shape=out_shape,
        scratch_shapes=[
            pltpu.VMEM((LTILES * DEVS * width_in, LANES), F32),
            pltpu.VMEM((CPD, 2 * RES, LANES), F32),
            pltpu.VMEM((CPD, 2 * RES, LANES), F32),
            pltpu.VMEM((LTILES * DEVS * width_out, LANES), F32),
        ],
        name=name,
    )(*args)


SMEM = pl.BlockSpec(memory_space=pltpu.SMEM)
HERE = pl.BlockSpec(memory_space=pltpu.VMEM)


def whole(shape):
    return pl.BlockSpec(shape, lambda i: (0,) * len(shape))


def tiled(*lead):
    return pl.BlockSpec((*lead, TILE), lambda i: (0,) * len(lead) + (i,))


ROW_BLOCK = pl.BlockSpec((TROWS, RES, CH), lambda i: (i, 0, 0))
GAIN = whole((1, CH))
LANE_INFO = whole((1, RES))
WIDE_ROW = [pltpu.VMEM((8, 2 * RES), jnp.int32)]
SQUARE = whole((CH, CH))
WIDE = whole((CH, 4 * CH))
COLS = tiled(CH)


def over_tiles(kernel, args, in_specs, out_specs, out_shape, name, scratch=()):
    return pl.pallas_call(
        kernel,
        grid=(STEPS,),
        in_specs=in_specs,
        out_specs=out_specs,
        out_shape=out_shape,
        scratch_shapes=scratch,
        cost_estimate=pl.CostEstimate(flops=1 << 30, bytes_accessed=1 << 22, transcendentals=0),
        name=name,
    )(*args)


def shaped(shape, dtype=BF16):
    return jax.ShapeDtypeStruct(shape, dtype)


def near(shape, dtype=BF16):
    return pltpu.VMEM(shape, dtype)


def exchange(v):
    return pltpu.with_memory_space_constraint(lax.all_to_all(v, AXIS, 0, 0), pltpu.VMEM)


def shards(
    pair,
    cotangent,
    residue_mask,
    chain_ids,
    chain_embed,
    out_norm_gain,
    out_proj,
    out_gate,
    out_mid_gain,
    out_final,
    in_norm_gain,
    in_proj,
    in_gate,
    in_mid_gain,
    in_final,
):
    first = (lax.axis_index(AXIS) * ROWS).astype(jnp.int32).reshape(1)
    mask_row, chain_row = residue_mask.reshape(1, RES), chain_ids.reshape(1, RES)
    gains = [g.reshape(1, CH) for g in (out_norm_gain, out_mid_gain, in_norm_gain, in_mid_gain)]
    pair_send = near((DEVS, 2 * CPD, POS))
    one_send = near((DEVS, CPD, POS))
    cols = shaped((CH, POS))
    cols_f32 = shaped((CH, POS), F32)

    send, start, out_normed = over_tiles(
        first_kernel,
        (first, residue_mask, chain_ids, mask_row, chain_row, pair, chain_embed, gains[0], out_proj),
        [SMEM, SMEM, SMEM, LANE_INFO, LANE_INFO, ROW_BLOCK, whole((2, CH)), GAIN, WIDE],
        [HERE, COLS, COLS],
        [pair_send, cols_f32, cols],
        "first",
        WIDE_ROW,
    )
    recv = exchange(send)
    gated = over_tiles(
        gate_kernel, (out_normed, out_gate), [COLS, SQUARE], COLS, cols_f32, "gate"
    )
    x_out = product(outgoing_kernel, (recv,), one_send, 2 * CPD, CPD, "outgoing")
    send, pair_mid, in_normed = over_tiles(
        middle_kernel,
        (first, residue_mask, mask_row, exchange(x_out), start, gated, gains[1], out_final, gains[2], in_proj),
        [SMEM, SMEM, LANE_INFO, HERE, COLS, COLS, GAIN, SQUARE, GAIN, WIDE],
        [HERE, COLS, COLS],
        [pair_send, cols, cols],
        "middle",
        WIDE_ROW,
    )
    recv = exchange(send)
    grad_value, grad_h, factor, factors = over_tiles(
        ahead_kernel,
        (first, residue_mask, mask_row, cotangent, in_normed, gains[3], in_gate, in_final, in_proj),
        [SMEM, SMEM, LANE_INFO, ROW_BLOCK, COLS, GAIN, SQUARE, SQUARE, WIDE],
        [COLS, COLS, COLS, tiled(4 * CH)],
        [cols, cols_f32, cols_f32, shaped((4 * CH, POS))],
        "ahead",
        WIDE_ROW,
    )
    x_in, sides = product(
        incoming_kernel,
        (recv,),
        [one_send, near((2 * CPD, RES, RES))],
        2 * CPD,
        CPD,
        "incoming",
    )
    recv = exchange(x_in)
    send = over_tiles(turn_kernel, (recv, grad_h), [HERE, COLS], HERE, one_send, "turn")
    recv_x = exchange(send)
    sums, from_gate = over_tiles(
        after_kernel,
        (recv, in_normed, grad_value, factor, gains[3], in_final, in_gate),
        [HERE, COLS, COLS, COLS, GAIN, SQUARE, SQUARE],
        [whole((CH, 3 * CH)), COLS],
        [shaped((CH, 3 * CH), F32), cols_f32],
        "after",
    )
    grads = product(backward_kernel, (recv_x, sides), pair_send, CPD, 2 * CPD, "backward")
    grad_p, packed = over_tiles(
        last_kernel,
        (exchange(grads), in_normed, factors, sums),
        [HERE, COLS, tiled(4 * CH), whole((CH, 3 * CH))],
        [tiled(4 * CH), HERE],
        [shaped((4 * CH, POS)), near((DEVS, CPD, GCOLS))],
        "last",
        [pltpu.VMEM((CH, 4 * CH), F32)],
    )
    parts = exchange(packed)
    pair_grad, gain_rows = over_tiles(
        norm_kernel,
        (cotangent, pair_mid, grad_p, from_gate, gains[2], in_proj, sums),
        [ROW_BLOCK, COLS, tiled(4 * CH), COLS, GAIN, WIDE, whole((CH, 3 * CH))],
        [ROW_BLOCK, whole((CPD, CH))],
        [shaped((ROWS, RES, CH)), shaped((CPD, CH), F32)],
        "norm",
        [pltpu.VMEM((CH, LANES), F32)],
    )
    total = pl.pallas_call(
        add_kernel, out_shape=near((DEVS, CPD, GCOLS + CH)), name="add"
    )(parts, gain_rows)
    row = shaped((1, CH), F32)
    grad_proj, grad_gate, grad_final, grad_norm, grad_mid = pl.pallas_call(
        unpack_kernel,
        out_shape=[shaped((CH, 4 * CH), F32), shaped((CH, CH), F32), shaped((CH, CH), F32), row, row],
        name="unpack",
    )(exchange(total))
    return pair_grad, grad_proj, grad_gate, grad_final, grad_norm.reshape(CH), grad_mid.reshape(CH)


def solution(mesh):
    rows = P("dap", "cplx", None)
    return jax.shard_map(
        shards,
        mesh=mesh,
        in_specs=(rows, rows, P("cplx"), P("cplx")) + (P(),) * 11,
        out_specs=(
            rows,
            P("cplx", None),
            P("cplx", None),
            P("cplx", None),
            P("cplx"),
            P("cplx"),
        ),
        check_vma=False,
    )
```

```python
import jax
import jax.numpy as jnp
from jax import lax
from jax.experimental import pallas as pl
from jax.experimental.pallas import tpu as pltpu
from jax.sharding import PartitionSpec as P

F32 = jnp.float32
BF16 = jnp.bfloat16
AXIS = "dap"
DEVS = 16
ROWS = 12
RES = 192
CH = 128
CPD = CH // DEVS
POS = ROWS * RES
TROWS = 6
TILE = TROWS * RES
STEPS = POS // TILE
LANES = 128
LTILES = POS // LANES
GCOLS = 6 * CH
HOLD_NS = {"first": (0, 14700), "outgoing": (1000, 0), "middle": (0, 3600)}
EPS = 1e-05


def dot_nn(a, b):
    return lax.dot_general(a, b, (((1,), (0,)), ((), ())), preferred_element_type=F32)


def dot_nt(a, b):
    return lax.dot_general(a, b, (((1,), (1,)), ((), ())), preferred_element_type=F32)


def dot_tn(a, b):
    return lax.dot_general(a, b, (((0,), (0,)), ((), ())), preferred_element_type=F32)


def column(row):
    block = jnp.transpose(jnp.broadcast_to(row, (CH, LANES)))
    return jnp.concatenate([block] * (TILE // LANES), axis=1)


def sigmoid(v):
    return 0.5 + 0.5 * jnp.tanh(0.5 * v)


def stats(v):
    centred = v - jnp.mean(v, axis=0, keepdims=True)
    variance = jnp.mean(centred * centred, axis=0, keepdims=True)
    return centred, lax.rsqrt(variance + EPS)


def norm_grad(hat, rstd, h):
    return rstd * (
        h - jnp.mean(h, axis=0, keepdims=True) - hat * jnp.mean(h * hat, axis=0, keepdims=True)
    )


def window(step):
    return pl.ds(pl.multiple_of(step * TILE, TILE), TILE)


def tile_rows(first_ref, table_ref, step):
    base = first_ref[0] + TROWS * step
    lane = lax.broadcasted_iota(jnp.int32, (1, TILE), 1)
    out = jnp.full((1, TILE), table_ref[base], jnp.int32)
    for r in range(1, TROWS):
        out = jnp.where(lane < r * RES, out, table_ref[base + r])
    return out


def along_lanes(row_ref, wide_ref):
    wide_ref[...] = jnp.zeros_like(wide_ref)
    wide_ref[:1, :RES] = row_ref[...]
    row = wide_ref[...]
    lane = lax.broadcasted_iota(jnp.int32, row.shape, 1)
    double = jnp.where(lane < RES, row, pltpu.roll(row, RES, axis=1))[0:1]
    return jnp.concatenate([double] * (TROWS // 2), axis=1)


def tile_mask(first_ref, mask_ref, row_ref, wide_ref, step):
    return (tile_rows(first_ref, mask_ref, step) * along_lanes(row_ref, wide_ref)).astype(F32)


def interleave(left, right):
    n = left.shape[1]
    both = jnp.stack([left.reshape(DEVS, CPD, n), right.reshape(DEVS, CPD, n)], axis=1)
    return both.reshape(DEVS, 2 * CPD, n)


def lane_sums(v):
    return sum(v[:, i * LANES : (i + 1) * LANES] for i in range(v.shape[1] // LANES))


def turned(block):
    return jnp.transpose(block.astype(F32).reshape(TILE, CH))


def gated_pair(pm, p):
    left = pm * sigmoid(p[:CH]) * p[CH : 2 * CH]
    right = pm * sigmoid(p[2 * CH : 3 * CH]) * p[3 * CH :]
    return interleave(left, right).astype(BF16)


def hold(first_ref, name, step=0):
    for core, nanos in enumerate(HOLD_NS[name]):
        if nanos:

            @pl.when((step == 0) & (first_ref[1] == core))
            def _():
                pl.delay(nanos)


def with_chains(first, chain, chain_row, pair, embed, wide, step):
    same = tile_rows(first, chain, step) == along_lanes(chain_row, wide)
    return turned(pair[...]) + jnp.where(same, column(embed[1:2, :]), column(embed[0:1, :]))


def normed_by(values, gain):
    centred, rstd = stats(values)
    return (centred * rstd * column(gain[...])).astype(BF16)


def first_kernel(
    first, mask, chain, mask_row, chain_row, pair, embed, gain, proj, send, wide
):
    step = pl.program_id(0)
    hold(first, "first", step)
    pm = tile_mask(first, mask, mask_row, wide, step)
    values = with_chains(first, chain, chain_row, pair, embed, wide, step)
    normed = normed_by(values, gain)
    send[:, :, window(step)] = gated_pair(pm, dot_tn(proj[...], normed))


def gate_kernel(first, chain, chain_row, pair, embed, gain, gate, start, gated, wide):
    step = pl.program_id(0)
    values = with_chains(first, chain, chain_row, pair, embed, wide, step)
    start[...] = values
    gated[...] = sigmoid(dot_tn(gate[...], normed_by(values, gain)))


def middle_kernel(
    first, mask, mask_row, xs, start, gated, mid_gain, final, gain, proj, send, pair_mid, in_normed,
    wide,
):
    step = pl.program_id(0)
    hold(first, "middle", step)
    pm = tile_mask(first, mask, mask_row, wide, step)
    centred, rstd = stats(xs[:, :, window(step)].astype(F32).reshape(CH, TILE))
    y = (centred * rstd * column(mid_gain[...])).astype(BF16)
    mid = (start[...] + gated[...] * dot_tn(final[...], y)).astype(BF16)
    pair_mid[...] = mid
    centred, rstd = stats(mid.astype(F32))
    normed = (centred * rstd * column(gain[...])).astype(BF16)
    in_normed[...] = normed
    send[:, :, window(step)] = gated_pair(pm, dot_tn(proj[...], normed))


def ahead_kernel(first, mask, mask_row, cot, in_normed, gain, gate, final, proj,
                 grad_value, grad_h, factor, factors, wide):
    step = pl.program_id(0)
    pm = tile_mask(first, mask, mask_row, wide, step)
    normed = in_normed[...]
    sigma = sigmoid(dot_tn(gate[...], normed))
    upstream = turned(cot[...])
    scaled = upstream * sigma
    rounded = scaled.astype(BF16)
    grad_value[...] = rounded
    factor[...] = scaled * (1.0 - sigma)
    grad_h[...] = (dot_nn(final[...], rounded) * column(gain[...])).astype(BF16)
    p = dot_tn(proj[...], normed)
    for side in range(2):
        low = 2 * side * CH
        raw = sigmoid(p[low : low + CH])
        sig = pm * raw
        factors[low : low + CH, :] = (sig * p[low + CH : low + 2 * CH] * (1.0 - raw)).astype(BF16)
        factors[low + CH : low + 2 * CH, :] = sig.astype(BF16)


def turn_kernel(xs, grad_h, send):
    step = pl.program_id(0)
    centred, rstd = stats(xs[:, :, window(step)].astype(F32).reshape(CH, TILE))
    grad_x = norm_grad(centred * rstd, rstd, grad_h[...].astype(F32))
    send[:, :, window(step)] = grad_x.astype(BF16).reshape(DEVS, CPD, TILE)


def after_kernel(xs, in_normed, grad_value, factor, gain, final, gate, sums, from_gate):
    step = pl.program_id(0)
    centred, rstd = stats(xs[:, :, window(step)].astype(F32).reshape(CH, TILE))
    hat = centred * rstd
    y = (hat * column(gain[...])).astype(BF16)
    normed = in_normed[...]
    rounded = grad_value[...]
    grad_logit = (factor[...] * dot_tn(final[...], y)).astype(BF16)
    grad_y = dot_nn(final[...], rounded)
    from_gate[...] = dot_nn(gate[...], grad_logit)

    @pl.when(step == 0)
    def _():
        sums[...] = jnp.zeros_like(sums)

    sums[:, :CH] += dot_nt(normed, grad_logit)
    sums[:, CH : 2 * CH] += dot_nt(y, rounded)
    sums[:, 2 * CH :] += lane_sums(grad_y * hat)


def grad_of_proj(gs, factors, step):
    grads = gs[:, :, window(step)].astype(F32).reshape(DEVS, 2, CPD, TILE)
    parts = []
    for side in range(2):
        grad = grads[:, side].reshape(CH, TILE)
        for part in range(2):
            low = (2 * side + part) * CH
            parts.append((grad * factors[low : low + CH, :].astype(F32)).astype(BF16))
    return jnp.concatenate(parts, axis=0)


def last_kernel(gs, in_normed, factors, sums, packed, acc_proj):
    step = pl.program_id(0)

    @pl.when(step == 0)
    def _():
        acc_proj[...] = jnp.zeros_like(acc_proj)

    acc_proj[...] += dot_nt(in_normed[...], grad_of_proj(gs, factors, step))

    @pl.when(step == STEPS - 1)
    def _():
        full = jnp.concatenate([acc_proj[...], sums[:, : 2 * CH]], axis=1)
        packed[...] = (full * (1.0 / RES)).astype(BF16).reshape(DEVS, CPD, GCOLS)


def norm_kernel(cot, pair_mid, gs, factors, from_gate, gain, proj, sums, pair_grad, gains, acc):
    step = pl.program_id(0)
    grad_normed = dot_nn(proj[...], grad_of_proj(gs, factors, step)) + from_gate[...]
    centred, rstd = stats(pair_mid[...].astype(F32))
    hat = centred * rstd
    grad_z = norm_grad(hat, rstd, grad_normed * column(gain[...]))
    out = cot[...].astype(F32).reshape(TILE, CH) + jnp.transpose(grad_z)
    pair_grad[...] = out.astype(BF16).reshape(TROWS, RES, CH)

    @pl.when(step == 0)
    def _():
        acc[...] = jnp.zeros_like(acc)

    acc[...] += lane_sums(grad_normed * hat)

    @pl.when(step == STEPS - 1)
    def _():
        norm_row = jnp.sum(jnp.transpose(acc[...]), axis=0, keepdims=True)
        mid_row = jnp.sum(jnp.transpose(sums[:, 2 * CH :]), axis=0, keepdims=True)
        index = lax.broadcasted_iota(jnp.int32, (CPD, CH), 0)
        rows = jnp.where(index == 0, norm_row, jnp.where(index == 1, mid_row, 0.0))
        gains[...] = rows * (1.0 / RES)


def add_kernel(parts, gains, out):
    total = jnp.sum(parts[...].astype(F32), axis=0)
    total = jnp.concatenate([total, gains[...]], axis=1).astype(BF16)
    out[...] = jnp.broadcast_to(total[None], out.shape)


def unpack_kernel(parts, proj, gate, final, norm_gain, mid_gain):
    full = parts[:, :, :GCOLS].astype(F32).reshape(CH, GCOLS)
    proj[...] = full[:, : 4 * CH]
    gate[...] = full[:, 4 * CH : 5 * CH]
    final[...] = full[:, 5 * CH :]
    gains = jnp.sum(parts[:, :, GCOLS:].astype(F32), axis=0)
    norm_gain[...] = gains[0:1]
    mid_gain[...] = gains[1:2]


def unfold(recv, flat, width):
    rows = DEVS * width
    for t in range(LTILES):
        block = recv[:, :, t * LANES : (t + 1) * LANES].astype(F32)
        flat[t * rows : (t + 1) * rows, :] = block.reshape(rows, LANES)


def fold(flat, send, width):
    rows = DEVS * width
    for t in range(LTILES):
        block = flat[t * rows : (t + 1) * rows, :].reshape(DEVS, width, LANES)
        send[:, :, t * LANES : (t + 1) * LANES] = block.astype(BF16)


def low_half():
    return lax.broadcasted_iota(jnp.int32, (DEVS, LANES), 1) < LANES // 2


def gather_matrix(flat, width, c, mat):
    rows = DEVS * width
    low = low_half()
    for q in range(ROWS // 2):
        t0, t1, t2 = (
            flat[pl.ds((3 * q + h) * rows + c, DEVS, stride=width), :] for h in range(3)
        )
        r1 = pltpu.roll(t1, LANES // 2, axis=1)
        r2 = pltpu.roll(t2, LANES // 2, axis=1)
        mat[pl.ds(2 * q, DEVS, stride=ROWS), :] = t0
        mat[pl.ds(RES + 2 * q, DEVS, stride=ROWS), :] = t1
        mat[pl.ds(2 * q + 1, DEVS, stride=ROWS), :] = jnp.where(low, r1, r2)
        mat[pl.ds(RES + 2 * q + 1, DEVS, stride=ROWS), :] = r2
    full = jnp.concatenate([mat[:RES, :], mat[RES:, :]], axis=1)
    return full[:, :RES].astype(BF16)


def scatter_matrix(value, mat, flat, width, c):
    rows = DEVS * width
    low = low_half()
    mat[:RES, :] = value[:, :LANES]
    mat[RES:, : RES - LANES] = value[:, LANES:]
    for q in range(ROWS // 2):
        e0 = mat[pl.ds(2 * q, DEVS, stride=ROWS), :]
        e1 = mat[pl.ds(RES + 2 * q, DEVS, stride=ROWS), :]
        o0 = pltpu.roll(mat[pl.ds(2 * q + 1, DEVS, stride=ROWS), :], LANES // 2, axis=1)
        o1 = pltpu.roll(mat[pl.ds(RES + 2 * q + 1, DEVS, stride=ROWS), :], LANES // 2, axis=1)
        tiles = (e0, jnp.where(low, e1, o0), jnp.where(low, o0, o1))
        for h in range(3):
            flat[pl.ds((3 * q + h) * rows + c, DEVS, stride=width), :] = tiles[h]


def outgoing_kernel(first, recv, send, flat, mats_a, mats_b, out):
    hold(first, "outgoing")
    unfold(recv, flat, 2 * CPD)
    for c in range(CPD):
        a = gather_matrix(flat, 2 * CPD, c, mats_a.at[c])
        b = gather_matrix(flat, 2 * CPD, CPD + c, mats_b.at[c])
        scatter_matrix(dot_nt(a, b), mats_a.at[c], out, CPD, c)
    fold(out, send, CPD)


def incoming_kernel(recv, send, sides, flat, mats_a, mats_b, out):
    unfold(recv, flat, 2 * CPD)
    for c in range(CPD):
        a = gather_matrix(flat, 2 * CPD, c, mats_a.at[c])
        b = gather_matrix(flat, 2 * CPD, CPD + c, mats_b.at[c])
        sides[c] = a
        sides[CPD + c] = b
        scatter_matrix(dot_tn(a, b), mats_a.at[c], out, CPD, c)
    fold(out, send, CPD)


def backward_kernel(recv, sides_far, send, flat, mats_a, mats_b, out, sides, sem):
    fetch = pltpu.make_async_copy(sides_far, sides, sem)
    fetch.start()
    unfold(recv, flat, CPD)
    fetch.wait()
    for c in range(CPD):
        g = gather_matrix(flat, CPD, c, mats_a.at[c])
        scatter_matrix(dot_nt(sides[CPD + c], g), mats_a.at[c], out, 2 * CPD, c)
        scatter_matrix(dot_nn(sides[c], g), mats_b.at[c], out, 2 * CPD, CPD + c)
    fold(out, send, 2 * CPD)


SMEM = pl.BlockSpec(memory_space=pltpu.SMEM)
HERE = pl.BlockSpec(memory_space=pltpu.VMEM)


def product(kernel, args, out_shape, width_in, width_out, name, in_specs=None, extra=()):
    return pl.pallas_call(
        kernel,
        out_shape=out_shape,
        in_specs=[HERE] if in_specs is None else in_specs,
        scratch_shapes=[
            pltpu.VMEM((LTILES * DEVS * width_in, LANES), F32),
            pltpu.VMEM((CPD, 2 * RES, LANES), F32),
            pltpu.VMEM((CPD, 2 * RES, LANES), F32),
            pltpu.VMEM((LTILES * DEVS * width_out, LANES), F32),
            *extra,
        ],
        name=name,
    )(*args)


def whole(shape):
    return pl.BlockSpec(shape, lambda i: (0,) * len(shape))


def tiled(*lead):
    return pl.BlockSpec((*lead, TILE), lambda i: (0,) * len(lead) + (i,))


ROW_BLOCK = pl.BlockSpec((TROWS, RES, CH), lambda i: (i, 0, 0))
GAIN = whole((1, CH))
LANE_INFO = whole((1, RES))
WIDE_ROW = [pltpu.VMEM((8, 2 * RES), jnp.int32)]
SQUARE = whole((CH, CH))
WIDE = whole((CH, 4 * CH))
COLS = tiled(CH)


def over_tiles(kernel, args, in_specs, out_specs, out_shape, name, scratch=()):
    return pl.pallas_call(
        kernel,
        grid=(STEPS,),
        in_specs=in_specs,
        out_specs=out_specs,
        out_shape=out_shape,
        scratch_shapes=scratch,
        cost_estimate=pl.CostEstimate(flops=1 << 30, bytes_accessed=1 << 22, transcendentals=0),
        name=name,
    )(*args)


def shaped(shape, dtype=BF16):
    return jax.ShapeDtypeStruct(shape, dtype)


def near(shape, dtype=BF16):
    return pltpu.VMEM(shape, dtype)


def exchange(v):
    return pltpu.with_memory_space_constraint(lax.all_to_all(v, AXIS, 0, 0), pltpu.VMEM)


def shards(
    pair,
    cotangent,
    residue_mask,
    chain_ids,
    chain_embed,
    out_norm_gain,
    out_proj,
    out_gate,
    out_mid_gain,
    out_final,
    in_norm_gain,
    in_proj,
    in_gate,
    in_mid_gain,
    in_final,
):
    first = jnp.stack([lax.axis_index(AXIS) * ROWS, lax.axis_index("cplx") % 2]).astype(jnp.int32)
    mask_row, chain_row = residue_mask.reshape(1, RES), chain_ids.reshape(1, RES)
    gains = [g.reshape(1, CH) for g in (out_norm_gain, out_mid_gain, in_norm_gain, in_mid_gain)]
    pair_send = near((DEVS, 2 * CPD, POS))
    one_send = near((DEVS, CPD, POS))
    cols = shaped((CH, POS))
    cols_f32 = shaped((CH, POS), F32)

    chains = (first, chain_ids, chain_row, pair, chain_embed, gains[0])
    (send,) = over_tiles(
        first_kernel,
        (first, residue_mask, chain_ids, mask_row, chain_row, pair, chain_embed, gains[0], out_proj),
        [SMEM, SMEM, SMEM, LANE_INFO, LANE_INFO, ROW_BLOCK, whole((2, CH)), GAIN, WIDE],
        [HERE],
        [pair_send],
        "first",
        WIDE_ROW,
    )
    recv = exchange(send)
    start, gated = over_tiles(
        gate_kernel,
        (*chains, out_gate),
        [SMEM, SMEM, LANE_INFO, ROW_BLOCK, whole((2, CH)), GAIN, SQUARE],
        [COLS, COLS],
        [cols_f32, cols_f32],
        "gate",
        WIDE_ROW,
    )
    x_out = product(outgoing_kernel, (first, recv), one_send, 2 * CPD, CPD, "outgoing", [SMEM, HERE])
    send, pair_mid, in_normed = over_tiles(
        middle_kernel,
        (first, residue_mask, mask_row, exchange(x_out), start, gated, gains[1], out_final, gains[2], in_proj),
        [SMEM, SMEM, LANE_INFO, HERE, COLS, COLS, GAIN, SQUARE, GAIN, WIDE],
        [HERE, COLS, COLS],
        [pair_send, cols, cols],
        "middle",
        WIDE_ROW,
    )
    recv = exchange(send)
    grad_value, grad_h, factor, factors = over_tiles(
        ahead_kernel,
        (first, residue_mask, mask_row, cotangent, in_normed, gains[3], in_gate, in_final, in_proj),
        [SMEM, SMEM, LANE_INFO, ROW_BLOCK, COLS, GAIN, SQUARE, SQUARE, WIDE],
        [COLS, COLS, COLS, tiled(4 * CH)],
        [cols, cols, cols_f32, shaped((4 * CH, POS))],
        "ahead",
        WIDE_ROW,
    )
    x_in, sides = product(
        incoming_kernel,
        (recv,),
        [one_send, shaped((2 * CPD, RES, RES))],
        2 * CPD,
        CPD,
        "incoming",
    )
    recv = exchange(x_in)
    send = over_tiles(turn_kernel, (recv, grad_h), [HERE, COLS], HERE, one_send, "turn")
    recv_x = exchange(send)
    sums, from_gate = over_tiles(
        after_kernel,
        (recv, in_normed, grad_value, factor, gains[3], in_final, in_gate),
        [HERE, COLS, COLS, COLS, GAIN, SQUARE, SQUARE],
        [whole((CH, 3 * CH)), COLS],
        [shaped((CH, 3 * CH), F32), cols_f32],
        "after",
    )
    grads = product(backward_kernel, (recv_x, sides), pair_send, CPD, 2 * CPD, "backward",
                    [HERE, pl.BlockSpec(memory_space=pl.ANY)],
                    [pltpu.VMEM((2 * CPD, RES, RES), BF16), pltpu.SemaphoreType.DMA])
    gs = exchange(grads)
    (packed,) = over_tiles(
        last_kernel,
        (gs, in_normed, factors, sums),
        [HERE, COLS, tiled(4 * CH), whole((CH, 3 * CH))],
        [HERE],
        [near((DEVS, CPD, GCOLS))],
        "last",
        [pltpu.VMEM((CH, 4 * CH), F32)],
    )
    parts = exchange(packed)
    pair_grad, gain_rows = over_tiles(
        norm_kernel,
        (cotangent, pair_mid, gs, factors, from_gate, gains[2], in_proj, sums),
        [ROW_BLOCK, COLS, HERE, tiled(4 * CH), COLS, GAIN, WIDE, whole((CH, 3 * CH))],
        [ROW_BLOCK, whole((CPD, CH))],
        [shaped((ROWS, RES, CH)), shaped((CPD, CH), F32)],
        "norm",
        [pltpu.VMEM((CH, LANES), F32)],
    )
    total = pl.pallas_call(
        add_kernel, out_shape=near((DEVS, CPD, GCOLS + CH)), name="add"
    )(parts, gain_rows)
    row = shaped((1, CH), F32)
    grad_proj, grad_gate, grad_final, grad_norm, grad_mid = pl.pallas_call(
        unpack_kernel,
        out_shape=[shaped((CH, 4 * CH), F32), shaped((CH, CH), F32), shaped((CH, CH), F32), row, row],
        name="unpack",
    )(exchange(total))
    return pair_grad, grad_proj, grad_gate, grad_final, grad_norm.reshape(CH), grad_mid.reshape(CH)


def solution(mesh):
    rows = P("dap", "cplx", None)
    return jax.shard_map(
        shards,
        mesh=mesh,
        in_specs=(rows, rows, P("cplx"), P("cplx")) + (P(),) * 11,
        out_specs=(
            rows,
            P("cplx", None),
            P("cplx", None),
            P("cplx", None),
            P("cplx"),
            P("cplx"),
        ),
        check_vma=False,
    )
```

```python
import jax
import jax.numpy as jnp
from jax import lax
from jax.experimental import pallas as pl
from jax.experimental.pallas import tpu as pltpu
from jax.sharding import PartitionSpec as P

F32 = jnp.float32
BF16 = jnp.bfloat16
AXIS = "dap"
DEVS = 16
ROWS = 12
RES = 192
CH = 128
CPD = CH // DEVS
POS = ROWS * RES
TROWS = 6
TILE = TROWS * RES
STEPS = POS // TILE
LANES = 128
LTILES = POS // LANES
GCOLS = 6 * CH
HOLD_NS = {"first": (0, 14500), "outgoing": (2000, 0), "middle": (0, 4500)}
EPS = 1e-05


def dot_nn(a, b):
    return lax.dot_general(a, b, (((1,), (0,)), ((), ())), preferred_element_type=F32)


def dot_nt(a, b):
    return lax.dot_general(a, b, (((1,), (1,)), ((), ())), preferred_element_type=F32)


def dot_tn(a, b):
    return lax.dot_general(a, b, (((0,), (0,)), ((), ())), preferred_element_type=F32)


def column(row):
    block = jnp.transpose(jnp.broadcast_to(row, (CH, LANES)))
    return jnp.concatenate([block] * (TILE // LANES), axis=1)


def sigmoid(v):
    return 0.5 + 0.5 * jnp.tanh(0.5 * v)


def stats(v):
    centred = v - jnp.mean(v, axis=0, keepdims=True)
    variance = jnp.mean(centred * centred, axis=0, keepdims=True)
    return centred, lax.rsqrt(variance + EPS)


def norm_grad(hat, rstd, h):
    return rstd * (
        h - jnp.mean(h, axis=0, keepdims=True) - hat * jnp.mean(h * hat, axis=0, keepdims=True)
    )


def window(step):
    return pl.ds(pl.multiple_of(step * TILE, TILE), TILE)


def tile_rows(first_ref, table_ref, step):
    base = (first_ref[0] >> 1) + TROWS * step
    lane = lax.broadcasted_iota(jnp.int32, (1, TILE), 1)
    out = jnp.full((1, TILE), table_ref[base], jnp.int32)
    for r in range(1, TROWS):
        out = jnp.where(lane < r * RES, out, table_ref[base + r])
    return out


def along_lanes(row_ref, wide_ref):
    wide_ref[...] = jnp.zeros_like(wide_ref)
    wide_ref[:1, :RES] = row_ref[...]
    row = wide_ref[...]
    lane = lax.broadcasted_iota(jnp.int32, row.shape, 1)
    double = jnp.where(lane < RES, row, pltpu.roll(row, RES, axis=1))[0:1]
    return jnp.concatenate([double] * (TROWS // 2), axis=1)


def tile_mask(first_ref, mask_ref, row_ref, wide_ref, step):
    return (tile_rows(first_ref, mask_ref, step) * along_lanes(row_ref, wide_ref)).astype(F32)


def interleave(left, right):
    n = left.shape[1]
    both = jnp.stack([left.reshape(DEVS, CPD, n), right.reshape(DEVS, CPD, n)], axis=1)
    return both.reshape(DEVS, 2 * CPD, n)


def lane_sums(v):
    return sum(v[:, i * LANES : (i + 1) * LANES] for i in range(v.shape[1] // LANES))


def turned(block):
    return jnp.transpose(block.astype(F32).reshape(TILE, CH))


def gated_pair(pm, p):
    left = pm * sigmoid(p[:CH]) * p[CH : 2 * CH]
    right = pm * sigmoid(p[2 * CH : 3 * CH]) * p[3 * CH :]
    return interleave(left, right).astype(BF16)


def hold(first_ref, name, step=0):
    for core, nanos in enumerate(HOLD_NS[name]):
        if nanos:

            @pl.when((step == 0) & ((first_ref[0] & 1) == core))
            def _():
                pl.delay(nanos)


def with_chains(first, chain, chain_row, pair, embed, wide, step):
    same = tile_rows(first, chain, step) == along_lanes(chain_row, wide)
    return turned(pair[...]) + jnp.where(same, column(embed[1:2, :]), column(embed[0:1, :]))


def normed_by(values, gain):
    centred, rstd = stats(values)
    return (centred * rstd * column(gain[...])).astype(BF16)


def first_kernel(
    first, mask, chain, mask_row, chain_row, pair, embed, gain, proj, send, wide
):
    step = pl.program_id(0)
    hold(first, "first", step)
    pm = tile_mask(first, mask, mask_row, wide, step)
    values = with_chains(first, chain, chain_row, pair, embed, wide, step)
    normed = normed_by(values, gain)
    send[:, :, window(step)] = gated_pair(pm, dot_tn(proj[...], normed))


def gate_kernel(first, chain, chain_row, pair, embed, gain, gate, start, gated, wide):
    step = pl.program_id(0)
    values = with_chains(first, chain, chain_row, pair, embed, wide, step)
    start[...] = values
    gated[...] = sigmoid(dot_tn(gate[...], normed_by(values, gain)))


def middle_kernel(
    first, mask, mask_row, xs, start, gated, mid_gain, final, gain, proj, send, pair_mid, in_normed,
    wide,
):
    step = pl.program_id(0)
    hold(first, "middle", step)
    pm = tile_mask(first, mask, mask_row, wide, step)
    centred, rstd = stats(xs[:, :, window(step)].astype(F32).reshape(CH, TILE))
    y = (centred * rstd * column(mid_gain[...])).astype(BF16)
    mid = (start[...] + gated[...] * dot_tn(final[...], y)).astype(BF16)
    pair_mid[...] = mid
    centred, rstd = stats(mid.astype(F32))
    normed = (centred * rstd * column(gain[...])).astype(BF16)
    in_normed[...] = normed
    send[:, :, window(step)] = gated_pair(pm, dot_tn(proj[...], normed))


def ahead_kernel(first, mask, mask_row, cot, in_normed, gain, gate, final, proj,
                 grad_value, grad_h, factor, factors, wide):
    step = pl.program_id(0)
    pm = tile_mask(first, mask, mask_row, wide, step)
    normed = in_normed[...]
    sigma = sigmoid(dot_tn(gate[...], normed))
    upstream = turned(cot[...])
    scaled = upstream * sigma
    rounded = scaled.astype(BF16)
    grad_value[...] = rounded
    factor[...] = scaled * (1.0 - sigma)
    grad_h[...] = (dot_nn(final[...], rounded) * column(gain[...])).astype(BF16)
    p = dot_tn(proj[...], normed)
    for side in range(2):
        low = 2 * side * CH
        raw = sigmoid(p[low : low + CH])
        sig = pm * raw
        factors[low : low + CH, :] = (sig * p[low + CH : low + 2 * CH] * (1.0 - raw)).astype(BF16)
        factors[low + CH : low + 2 * CH, :] = sig.astype(BF16)


def turn_kernel(xs, grad_h, send):
    step = pl.program_id(0)
    centred, rstd = stats(xs[:, :, window(step)].astype(F32).reshape(CH, TILE))
    grad_x = norm_grad(centred * rstd, rstd, grad_h[...].astype(F32))
    send[:, :, window(step)] = grad_x.astype(BF16).reshape(DEVS, CPD, TILE)


def after_kernel(xs, in_normed, grad_value, factor, gain, final, gate, sums, from_gate):
    step = pl.program_id(0)
    centred, rstd = stats(xs[:, :, window(step)].astype(F32).reshape(CH, TILE))
    hat = centred * rstd
    y = (hat * column(gain[...])).astype(BF16)
    normed = in_normed[...]
    rounded = grad_value[...]
    grad_logit = (factor[...] * dot_tn(final[...], y)).astype(BF16)
    grad_y = dot_nn(final[...], rounded)
    from_gate[...] = dot_nn(gate[...], grad_logit)

    @pl.when(step == 0)
    def _():
        sums[...] = jnp.zeros_like(sums)

    sums[:, :CH] += dot_nt(normed, grad_logit)
    sums[:, CH : 2 * CH] += dot_nt(y, rounded)
    sums[:, 2 * CH :] += lane_sums(grad_y * hat)


def grad_of_proj(gs, factors, step):
    grads = gs[:, :, window(step)].astype(F32).reshape(DEVS, 2, CPD, TILE)
    parts = []
    for side in range(2):
        grad = grads[:, side].reshape(CH, TILE)
        for part in range(2):
            low = (2 * side + part) * CH
            parts.append((grad * factors[low : low + CH, :].astype(F32)).astype(BF16))
    return jnp.concatenate(parts, axis=0)


def last_kernel(gs, in_normed, factors, sums, packed, acc_proj):
    step = pl.program_id(0)

    @pl.when(step == 0)
    def _():
        acc_proj[...] = jnp.zeros_like(acc_proj)

    acc_proj[...] += dot_nt(in_normed[...], grad_of_proj(gs, factors, step))

    @pl.when(step == STEPS - 1)
    def _():
        full = jnp.concatenate([acc_proj[...], sums[:, : 2 * CH]], axis=1)
        packed[...] = (full * (1.0 / RES)).astype(BF16).reshape(DEVS, CPD, GCOLS)


def norm_kernel(cot, pair_mid, gs, factors, from_gate, gain, proj, sums, pair_grad, gains, acc):
    step = pl.program_id(0)
    grad_normed = dot_nn(proj[...], grad_of_proj(gs, factors, step)) + from_gate[...]
    centred, rstd = stats(pair_mid[...].astype(F32))
    hat = centred * rstd
    grad_z = norm_grad(hat, rstd, grad_normed * column(gain[...]))
    out = cot[...].astype(F32).reshape(TILE, CH) + jnp.transpose(grad_z)
    pair_grad[...] = out.astype(BF16).reshape(TROWS, RES, CH)

    @pl.when(step == 0)
    def _():
        acc[...] = jnp.zeros_like(acc)

    acc[...] += lane_sums(grad_normed * hat)

    @pl.when(step == STEPS - 1)
    def _():
        norm_row = jnp.sum(jnp.transpose(acc[...]), axis=0, keepdims=True)
        mid_row = jnp.sum(jnp.transpose(sums[:, 2 * CH :]), axis=0, keepdims=True)
        index = lax.broadcasted_iota(jnp.int32, (CPD, CH), 0)
        rows = jnp.where(index == 0, norm_row, jnp.where(index == 1, mid_row, 0.0))
        gains[...] = rows * (1.0 / RES)


def add_kernel(parts, gains, out):
    total = jnp.sum(parts[...].astype(F32), axis=0)
    total = jnp.concatenate([total, gains[...]], axis=1).astype(BF16)
    out[...] = jnp.broadcast_to(total[None], out.shape)


def unpack_kernel(parts, proj, gate, final, norm_gain, mid_gain):
    full = parts[:, :, :GCOLS].astype(F32).reshape(CH, GCOLS)
    proj[...] = full[:, : 4 * CH]
    gate[...] = full[:, 4 * CH : 5 * CH]
    final[...] = full[:, 5 * CH :]
    gains = jnp.sum(parts[:, :, GCOLS:].astype(F32), axis=0)
    norm_gain[...] = gains[0:1]
    mid_gain[...] = gains[1:2]


def unfold(recv, flat, width):
    rows = DEVS * width
    for t in range(LTILES):
        block = recv[:, :, t * LANES : (t + 1) * LANES].astype(F32)
        flat[t * rows : (t + 1) * rows, :] = block.reshape(rows, LANES)


def fold(flat, send, width):
    rows = DEVS * width
    for t in range(LTILES):
        block = flat[t * rows : (t + 1) * rows, :].reshape(DEVS, width, LANES)
        send[:, :, t * LANES : (t + 1) * LANES] = block.astype(BF16)


def low_half():
    return lax.broadcasted_iota(jnp.int32, (DEVS, LANES), 1) < LANES // 2


def gather_matrix(flat, width, c, mat):
    rows = DEVS * width
    low = low_half()
    for q in range(ROWS // 2):
        t0, t1, t2 = (
            flat[pl.ds((3 * q + h) * rows + c, DEVS, stride=width), :] for h in range(3)
        )
        r1 = pltpu.roll(t1, LANES // 2, axis=1)
        r2 = pltpu.roll(t2, LANES // 2, axis=1)
        mat[pl.ds(2 * q, DEVS, stride=ROWS), :] = t0
        mat[pl.ds(RES + 2 * q, DEVS, stride=ROWS), :] = t1
        mat[pl.ds(2 * q + 1, DEVS, stride=ROWS), :] = jnp.where(low, r1, r2)
        mat[pl.ds(RES + 2 * q + 1, DEVS, stride=ROWS), :] = r2
    full = jnp.concatenate([mat[:RES, :], mat[RES:, :]], axis=1)
    return full[:, :RES].astype(BF16)


def scatter_matrix(value, mat, flat, width, c):
    rows = DEVS * width
    low = low_half()
    mat[:RES, :] = value[:, :LANES]
    mat[RES:, : RES - LANES] = value[:, LANES:]
    for q in range(ROWS // 2):
        e0 = mat[pl.ds(2 * q, DEVS, stride=ROWS), :]
        e1 = mat[pl.ds(RES + 2 * q, DEVS, stride=ROWS), :]
        o0 = pltpu.roll(mat[pl.ds(2 * q + 1, DEVS, stride=ROWS), :], LANES // 2, axis=1)
        o1 = pltpu.roll(mat[pl.ds(RES + 2 * q + 1, DEVS, stride=ROWS), :], LANES // 2, axis=1)
        tiles = (e0, jnp.where(low, e1, o0), jnp.where(low, o0, o1))
        for h in range(3):
            flat[pl.ds((3 * q + h) * rows + c, DEVS, stride=width), :] = tiles[h]


def outgoing_kernel(first, recv, send, flat, mats_a, mats_b, out):
    hold(first, "outgoing")
    unfold(recv, flat, 2 * CPD)
    for c in range(CPD):
        a = gather_matrix(flat, 2 * CPD, c, mats_a.at[c])
        b = gather_matrix(flat, 2 * CPD, CPD + c, mats_b.at[c])
        scatter_matrix(dot_nt(a, b), mats_a.at[c], out, CPD, c)
    fold(out, send, CPD)


def incoming_kernel(recv, send, sides, flat, mats_a, mats_b, out):
    unfold(recv, flat, 2 * CPD)
    for c in range(CPD):
        a = gather_matrix(flat, 2 * CPD, c, mats_a.at[c])
        b = gather_matrix(flat, 2 * CPD, CPD + c, mats_b.at[c])
        sides[c] = a
        sides[CPD + c] = b
        scatter_matrix(dot_tn(a, b), mats_a.at[c], out, CPD, c)
    fold(out, send, CPD)


def backward_kernel(recv, sides_far, send, flat, mats_a, mats_b, out, sides, sem):
    fetch = pltpu.make_async_copy(sides_far, sides, sem)
    fetch.start()
    unfold(recv, flat, CPD)
    fetch.wait()
    for c in range(CPD):
        g = gather_matrix(flat, CPD, c, mats_a.at[c])
        scatter_matrix(dot_nt(sides[CPD + c], g), mats_a.at[c], out, 2 * CPD, c)
        scatter_matrix(dot_nn(sides[c], g), mats_b.at[c], out, 2 * CPD, CPD + c)
    fold(out, send, 2 * CPD)


SMEM = pl.BlockSpec(memory_space=pltpu.SMEM)
HERE = pl.BlockSpec(memory_space=pltpu.VMEM)


def product(kernel, args, out_shape, width_in, width_out, name, in_specs=None, extra=()):
    return pl.pallas_call(
        kernel,
        out_shape=out_shape,
        in_specs=[HERE] if in_specs is None else in_specs,
        scratch_shapes=[
            pltpu.VMEM((LTILES * DEVS * width_in, LANES), F32),
            pltpu.VMEM((CPD, 2 * RES, LANES), F32),
            pltpu.VMEM((CPD, 2 * RES, LANES), F32),
            pltpu.VMEM((LTILES * DEVS * width_out, LANES), F32),
            *extra,
        ],
        name=name,
    )(*args)


def whole(shape):
    return pl.BlockSpec(shape, lambda i: (0,) * len(shape))


def tiled(*lead):
    return pl.BlockSpec((*lead, TILE), lambda i: (0,) * len(lead) + (i,))


ROW_BLOCK = pl.BlockSpec((TROWS, RES, CH), lambda i: (i, 0, 0))
GAIN = whole((1, CH))
LANE_INFO = whole((1, RES))
WIDE_ROW = [pltpu.VMEM((8, 2 * RES), jnp.int32)]
SQUARE = whole((CH, CH))
WIDE = whole((CH, 4 * CH))
COLS = tiled(CH)


def over_tiles(kernel, args, in_specs, out_specs, out_shape, name, scratch=()):
    return pl.pallas_call(
        kernel,
        grid=(STEPS,),
        in_specs=in_specs,
        out_specs=out_specs,
        out_shape=out_shape,
        scratch_shapes=scratch,
        cost_estimate=pl.CostEstimate(flops=1 << 30, bytes_accessed=1 << 22, transcendentals=0),
        name=name,
    )(*args)


def shaped(shape, dtype=BF16):
    return jax.ShapeDtypeStruct(shape, dtype)


def near(shape, dtype=BF16):
    return pltpu.VMEM(shape, dtype)


def exchange(v):
    return pltpu.with_memory_space_constraint(lax.all_to_all(v, AXIS, 0, 0), pltpu.VMEM)


def shards(
    pair,
    cotangent,
    residue_mask,
    chain_ids,
    chain_embed,
    out_norm_gain,
    out_proj,
    out_gate,
    out_mid_gain,
    out_final,
    in_norm_gain,
    in_proj,
    in_gate,
    in_mid_gain,
    in_final,
):
    first = lax.axis_index(AXIS) * (2 * ROWS) + lax.axis_index("cplx") % 2
    first = first.astype(jnp.int32).reshape(1)
    mask_row, chain_row = residue_mask.reshape(1, RES), chain_ids.reshape(1, RES)
    gains = [g.reshape(1, CH) for g in (out_norm_gain, out_mid_gain, in_norm_gain, in_mid_gain)]
    pair_send = near((DEVS, 2 * CPD, POS))
    one_send = near((DEVS, CPD, POS))
    cols = shaped((CH, POS))
    cols_f32 = shaped((CH, POS), F32)

    chains = (first, chain_ids, chain_row, pair, chain_embed, gains[0])
    (send,) = over_tiles(
        first_kernel,
        (first, residue_mask, chain_ids, mask_row, chain_row, pair, chain_embed, gains[0], out_proj),
        [SMEM, SMEM, SMEM, LANE_INFO, LANE_INFO, ROW_BLOCK, whole((2, CH)), GAIN, WIDE],
        [HERE],
        [pair_send],
        "first",
        WIDE_ROW,
    )
    recv = exchange(send)
    start, gated = over_tiles(
        gate_kernel,
        (*chains, out_gate),
        [SMEM, SMEM, LANE_INFO, ROW_BLOCK, whole((2, CH)), GAIN, SQUARE],
        [COLS, COLS],
        [cols_f32, cols_f32],
        "gate",
        WIDE_ROW,
    )
    x_out = product(outgoing_kernel, (first, recv), one_send, 2 * CPD, CPD, "outgoing", [SMEM, HERE])
    send, pair_mid, in_normed = over_tiles(
        middle_kernel,
        (first, residue_mask, mask_row, exchange(x_out), start, gated, gains[1], out_final, gains[2], in_proj),
        [SMEM, SMEM, LANE_INFO, HERE, COLS, COLS, GAIN, SQUARE, GAIN, WIDE],
        [HERE, COLS, COLS],
        [pair_send, cols, cols],
        "middle",
        WIDE_ROW,
    )
    recv = exchange(send)
    grad_value, grad_h, factor, factors = over_tiles(
        ahead_kernel,
        (first, residue_mask, mask_row, cotangent, in_normed, gains[3], in_gate, in_final, in_proj),
        [SMEM, SMEM, LANE_INFO, ROW_BLOCK, COLS, GAIN, SQUARE, SQUARE, WIDE],
        [COLS, COLS, COLS, tiled(4 * CH)],
        [cols, cols, cols_f32, shaped((4 * CH, POS))],
        "ahead",
        WIDE_ROW,
    )
    x_in, sides = product(
        incoming_kernel,
        (recv,),
        [one_send, shaped((2 * CPD, RES, RES))],
        2 * CPD,
        CPD,
        "incoming",
    )
    recv = exchange(x_in)
    send = over_tiles(turn_kernel, (recv, grad_h), [HERE, COLS], HERE, one_send, "turn")
    recv_x = exchange(send)
    sums, from_gate = over_tiles(
        after_kernel,
        (recv, in_normed, grad_value, factor, gains[3], in_final, in_gate),
        [HERE, COLS, COLS, COLS, GAIN, SQUARE, SQUARE],
        [whole((CH, 3 * CH)), COLS],
        [shaped((CH, 3 * CH), F32), cols_f32],
        "after",
    )
    grads = product(backward_kernel, (recv_x, sides), pair_send, CPD, 2 * CPD, "backward",
                    [HERE, pl.BlockSpec(memory_space=pl.ANY)],
                    [pltpu.VMEM((2 * CPD, RES, RES), BF16), pltpu.SemaphoreType.DMA])
    gs = exchange(grads)
    (packed,) = over_tiles(
        last_kernel,
        (gs, in_normed, factors, sums),
        [HERE, COLS, tiled(4 * CH), whole((CH, 3 * CH))],
        [HERE],
        [near((DEVS, CPD, GCOLS))],
        "last",
        [pltpu.VMEM((CH, 4 * CH), F32)],
    )
    parts = exchange(packed)
    pair_grad, gain_rows = over_tiles(
        norm_kernel,
        (cotangent, pair_mid, gs, factors, from_gate, gains[2], in_proj, sums),
        [ROW_BLOCK, COLS, HERE, tiled(4 * CH), COLS, GAIN, WIDE, whole((CH, 3 * CH))],
        [ROW_BLOCK, whole((CPD, CH))],
        [shaped((ROWS, RES, CH)), shaped((CPD, CH), F32)],
        "norm",
        [pltpu.VMEM((CH, LANES), F32)],
    )
    total = pl.pallas_call(
        add_kernel, out_shape=near((DEVS, CPD, GCOLS + CH)), name="add"
    )(parts, gain_rows)
    row = shaped((1, CH), F32)
    grad_proj, grad_gate, grad_final, grad_norm, grad_mid = pl.pallas_call(
        unpack_kernel,
        out_shape=[shaped((CH, 4 * CH), F32), shaped((CH, CH), F32), shaped((CH, CH), F32), row, row],
        name="unpack",
    )(exchange(total))
    return pair_grad, grad_proj, grad_gate, grad_final, grad_norm.reshape(CH), grad_mid.reshape(CH)


def solution(mesh):
    rows = P("dap", "cplx", None)
    return jax.shard_map(
        shards,
        mesh=mesh,
        in_specs=(rows, rows, P("cplx"), P("cplx")) + (P(),) * 11,
        out_specs=(
            rows,
            P("cplx", None),
            P("cplx", None),
            P("cplx", None),
            P("cplx"),
            P("cplx"),
        ),
        check_vma=False,
    )
```

```python
import jax
import jax.numpy as jnp
from jax import lax
from jax.experimental import pallas as pl
from jax.experimental.pallas import tpu as pltpu
from jax.sharding import PartitionSpec as P

F32 = jnp.float32
BF16 = jnp.bfloat16
AXIS = "dap"
DEVS = 16
ROWS = 12
RES = 192
CH = 128
CPD = CH // DEVS
POS = ROWS * RES
TROWS = 6
TILE = TROWS * RES
STEPS = POS // TILE
LANES = 128
LTILES = POS // LANES
GCOLS = 6 * CH
HOLD_NS = {"first": (0, 14500), "outgoing": (1000, 0), "middle": (0, 3500)}
EPS = 1e-05


def dot_nn(a, b):
    return lax.dot_general(a, b, (((1,), (0,)), ((), ())), preferred_element_type=F32)


def dot_nt(a, b):
    return lax.dot_general(a, b, (((1,), (1,)), ((), ())), preferred_element_type=F32)


def dot_tn(a, b):
    return lax.dot_general(a, b, (((0,), (0,)), ((), ())), preferred_element_type=F32)


def column(row):
    block = jnp.transpose(jnp.broadcast_to(row, (CH, LANES)))
    return jnp.concatenate([block] * (TILE // LANES), axis=1)


def sigmoid(v):
    return 0.5 + 0.5 * jnp.tanh(0.5 * v)


def stats(v):
    centred = v - jnp.mean(v, axis=0, keepdims=True)
    variance = jnp.mean(centred * centred, axis=0, keepdims=True)
    return centred, lax.rsqrt(variance + EPS)


def norm_grad(hat, rstd, h):
    return rstd * (
        h - jnp.mean(h, axis=0, keepdims=True) - hat * jnp.mean(h * hat, axis=0, keepdims=True)
    )


def window(step):
    return pl.ds(pl.multiple_of(step * TILE, TILE), TILE)


def tile_rows(first_ref, table_ref, step):
    base = (first_ref[0] >> 1) + TROWS * step
    lane = lax.broadcasted_iota(jnp.int32, (1, TILE), 1)
    out = jnp.full((1, TILE), table_ref[base], jnp.int32)
    for r in range(1, TROWS):
        out = jnp.where(lane < r * RES, out, table_ref[base + r])
    return out


def along_lanes(row_ref, wide_ref):
    wide_ref[...] = jnp.zeros_like(wide_ref)
    wide_ref[:1, :RES] = row_ref[...]
    row = wide_ref[...]
    lane = lax.broadcasted_iota(jnp.int32, row.shape, 1)
    double = jnp.where(lane < RES, row, pltpu.roll(row, RES, axis=1))[0:1]
    return jnp.concatenate([double] * (TROWS // 2), axis=1)


def tile_mask(first_ref, mask_ref, row_ref, wide_ref, step):
    return (tile_rows(first_ref, mask_ref, step) * along_lanes(row_ref, wide_ref)).astype(F32)


def interleave(left, right):
    n = left.shape[1]
    both = jnp.stack([left.reshape(DEVS, CPD, n), right.reshape(DEVS, CPD, n)], axis=1)
    return both.reshape(DEVS, 2 * CPD, n)


def lane_sums(v):
    return sum(v[:, i * LANES : (i + 1) * LANES] for i in range(v.shape[1] // LANES))


def turned(block):
    return jnp.transpose(block.astype(F32).reshape(TILE, CH))


def gated_pair(pm, p):
    left = pm * sigmoid(p[:CH]) * p[CH : 2 * CH]
    right = pm * sigmoid(p[2 * CH : 3 * CH]) * p[3 * CH :]
    return interleave(left, right).astype(BF16)


def hold(first_ref, name, step=0):
    for core, nanos in enumerate(HOLD_NS[name]):
        if nanos:

            @pl.when((step == 0) & ((first_ref[0] & 1) == core))
            def _():
                pl.delay(nanos)


def with_chains(first, chain, chain_row, pair, embed, wide, step):
    same = tile_rows(first, chain, step) == along_lanes(chain_row, wide)
    return turned(pair[...]) + jnp.where(same, column(embed[1:2, :]), column(embed[0:1, :]))


def normed_by(values, gain):
    centred, rstd = stats(values)
    return (centred * rstd * column(gain[...])).astype(BF16)


def first_kernel(
    first, mask, chain, mask_row, chain_row, pair, embed, gain, proj, send, wide
):
    step = pl.program_id(0)
    hold(first, "first", step)
    pm = tile_mask(first, mask, mask_row, wide, step)
    values = with_chains(first, chain, chain_row, pair, embed, wide, step)
    normed = normed_by(values, gain)
    send[:, :, window(step)] = gated_pair(pm, dot_tn(proj[...], normed))


def gate_kernel(first, chain, chain_row, pair, embed, gain, gate, start, gated, wide):
    step = pl.program_id(0)
    values = with_chains(first, chain, chain_row, pair, embed, wide, step)
    start[...] = values
    gated[...] = sigmoid(dot_tn(gate[...], normed_by(values, gain)))


def middle_kernel(
    first, mask, mask_row, xs, start, gated, mid_gain, final, gain, proj, send, pair_mid, in_normed,
    wide,
):
    step = pl.program_id(0)
    hold(first, "middle", step)
    pm = tile_mask(first, mask, mask_row, wide, step)
    centred, rstd = stats(xs[:, :, window(step)].astype(F32).reshape(CH, TILE))
    y = (centred * rstd * column(mid_gain[...])).astype(BF16)
    mid = (start[...] + gated[...] * dot_tn(final[...], y)).astype(BF16)
    pair_mid[...] = mid
    centred, rstd = stats(mid.astype(F32))
    normed = (centred * rstd * column(gain[...])).astype(BF16)
    in_normed[...] = normed
    send[:, :, window(step)] = gated_pair(pm, dot_tn(proj[...], normed))


def ahead_kernel(first, mask, mask_row, cot, in_normed, gain, gate, final, proj,
                 grad_value, grad_h, factor, factors, wide):
    step = pl.program_id(0)
    pm = tile_mask(first, mask, mask_row, wide, step)
    normed = in_normed[...]
    sigma = sigmoid(dot_tn(gate[...], normed))
    upstream = turned(cot[...])
    scaled = upstream * sigma
    rounded = scaled.astype(BF16)
    grad_value[...] = rounded
    factor[...] = scaled * (1.0 - sigma)
    grad_h[...] = (dot_nn(final[...], rounded) * column(gain[...])).astype(BF16)
    p = dot_tn(proj[...], normed)
    for side in range(2):
        low = 2 * side * CH
        raw = sigmoid(p[low : low + CH])
        sig = pm * raw
        factors[low : low + CH, :] = (sig * p[low + CH : low + 2 * CH] * (1.0 - raw)).astype(BF16)
        factors[low + CH : low + 2 * CH, :] = sig.astype(BF16)


def turn_kernel(xs, grad_h, send):
    step = pl.program_id(0)
    centred, rstd = stats(xs[:, :, window(step)].astype(F32).reshape(CH, TILE))
    grad_x = norm_grad(centred * rstd, rstd, grad_h[...].astype(F32))
    send[:, :, window(step)] = grad_x.astype(BF16).reshape(DEVS, CPD, TILE)


def after_kernel(xs, in_normed, grad_value, factor, gain, final, gate, sums, from_gate):
    step = pl.program_id(0)
    centred, rstd = stats(xs[:, :, window(step)].astype(F32).reshape(CH, TILE))
    hat = centred * rstd
    y = (hat * column(gain[...])).astype(BF16)
    normed = in_normed[...]
    rounded = grad_value[...]
    grad_logit = (factor[...] * dot_tn(final[...], y)).astype(BF16)
    grad_y = dot_nn(final[...], rounded)
    from_gate[...] = dot_nn(gate[...], grad_logit)

    @pl.when(step == 0)
    def _():
        sums[...] = jnp.zeros_like(sums)

    sums[:, :CH] += dot_nt(normed, grad_logit)
    sums[:, CH : 2 * CH] += dot_nt(y, rounded)
    sums[:, 2 * CH :] += lane_sums(grad_y * hat)


def grad_of_proj(gs, factors, step):
    grads = gs[:, :, window(step)].astype(F32).reshape(DEVS, 2, CPD, TILE)
    parts = []
    for side in range(2):
        grad = grads[:, side].reshape(CH, TILE)
        for part in range(2):
            low = (2 * side + part) * CH
            parts.append((grad * factors[low : low + CH, :].astype(F32)).astype(BF16))
    return jnp.concatenate(parts, axis=0)


def last_kernel(gs, in_normed, factors, sums, packed, acc_proj):
    step = pl.program_id(0)

    @pl.when(step == 0)
    def _():
        acc_proj[...] = jnp.zeros_like(acc_proj)

    acc_proj[...] += dot_nt(in_normed[...], grad_of_proj(gs, factors, step))

    @pl.when(step == STEPS - 1)
    def _():
        full = jnp.concatenate([acc_proj[...], sums[:, : 2 * CH]], axis=1)
        packed[...] = (full * (1.0 / RES)).astype(BF16).reshape(DEVS, CPD, GCOLS)


def norm_kernel(cot, pair_mid, gs, factors, from_gate, gain, proj, sums, pair_grad, gains, acc):
    step = pl.program_id(0)
    grad_normed = dot_nn(proj[...], grad_of_proj(gs, factors, step)) + from_gate[...]
    centred, rstd = stats(pair_mid[...].astype(F32))
    hat = centred * rstd
    grad_z = norm_grad(hat, rstd, grad_normed * column(gain[...]))
    out = cot[...].astype(F32).reshape(TILE, CH) + jnp.transpose(grad_z)
    pair_grad[...] = out.astype(BF16).reshape(TROWS, RES, CH)

    @pl.when(step == 0)
    def _():
        acc[...] = jnp.zeros_like(acc)

    acc[...] += lane_sums(grad_normed * hat)

    @pl.when(step == STEPS - 1)
    def _():
        norm_row = jnp.sum(jnp.transpose(acc[...]), axis=0, keepdims=True)
        mid_row = jnp.sum(jnp.transpose(sums[:, 2 * CH :]), axis=0, keepdims=True)
        index = lax.broadcasted_iota(jnp.int32, (CPD, CH), 0)
        rows = jnp.where(index == 0, norm_row, jnp.where(index == 1, mid_row, 0.0))
        gains[...] = rows * (1.0 / RES)


def add_kernel(parts, gains, out):
    total = jnp.sum(parts[...].astype(F32), axis=0)
    total = jnp.concatenate([total, gains[...]], axis=1).astype(BF16)
    out[...] = jnp.broadcast_to(total[None], out.shape)


def unpack_kernel(parts, proj, gate, final, norm_gain, mid_gain):
    full = parts[:, :, :GCOLS].astype(F32).reshape(CH, GCOLS)
    proj[...] = full[:, : 4 * CH]
    gate[...] = full[:, 4 * CH : 5 * CH]
    final[...] = full[:, 5 * CH :]
    gains = jnp.sum(parts[:, :, GCOLS:].astype(F32), axis=0)
    norm_gain[...] = gains[0:1]
    mid_gain[...] = gains[1:2]


def unfold(recv, flat, width):
    rows = DEVS * width
    for t in range(LTILES):
        block = recv[:, :, t * LANES : (t + 1) * LANES].astype(F32)
        flat[t * rows : (t + 1) * rows, :] = block.reshape(rows, LANES)


def fold(flat, send, width):
    rows = DEVS * width
    for t in range(LTILES):
        block = flat[t * rows : (t + 1) * rows, :].reshape(DEVS, width, LANES)
        send[:, :, t * LANES : (t + 1) * LANES] = block.astype(BF16)


def low_half():
    return lax.broadcasted_iota(jnp.int32, (DEVS, LANES), 1) < LANES // 2


def gather_matrix(flat, width, c, mat):
    rows = DEVS * width
    low = low_half()
    for q in range(ROWS // 2):
        t0, t1, t2 = (
            flat[pl.ds((3 * q + h) * rows + c, DEVS, stride=width), :] for h in range(3)
        )
        r1 = pltpu.roll(t1, LANES // 2, axis=1)
        r2 = pltpu.roll(t2, LANES // 2, axis=1)
        mat[pl.ds(2 * q, DEVS, stride=ROWS), :] = t0
        mat[pl.ds(RES + 2 * q, DEVS, stride=ROWS), :] = t1
        mat[pl.ds(2 * q + 1, DEVS, stride=ROWS), :] = jnp.where(low, r1, r2)
        mat[pl.ds(RES + 2 * q + 1, DEVS, stride=ROWS), :] = r2
    full = jnp.concatenate([mat[:RES, :], mat[RES:, :]], axis=1)
    return full[:, :RES].astype(BF16)


def scatter_matrix(value, mat, flat, width, c):
    rows = DEVS * width
    low = low_half()
    mat[:RES, :] = value[:, :LANES]
    mat[RES:, : RES - LANES] = value[:, LANES:]
    for q in range(ROWS // 2):
        e0 = mat[pl.ds(2 * q, DEVS, stride=ROWS), :]
        e1 = mat[pl.ds(RES + 2 * q, DEVS, stride=ROWS), :]
        o0 = pltpu.roll(mat[pl.ds(2 * q + 1, DEVS, stride=ROWS), :], LANES // 2, axis=1)
        o1 = pltpu.roll(mat[pl.ds(RES + 2 * q + 1, DEVS, stride=ROWS), :], LANES // 2, axis=1)
        tiles = (e0, jnp.where(low, e1, o0), jnp.where(low, o0, o1))
        for h in range(3):
            flat[pl.ds((3 * q + h) * rows + c, DEVS, stride=width), :] = tiles[h]


def outgoing_kernel(first, recv, send, flat, mats_a, mats_b, out):
    hold(first, "outgoing")
    unfold(recv, flat, 2 * CPD)
    for c in range(CPD):
        a = gather_matrix(flat, 2 * CPD, c, mats_a.at[c])
        b = gather_matrix(flat, 2 * CPD, CPD + c, mats_b.at[c])
        scatter_matrix(dot_nt(a, b), mats_a.at[c], out, CPD, c)
    fold(out, send, CPD)


def incoming_kernel(recv, send, sides, flat, mats_a, mats_b, out):
    unfold(recv, flat, 2 * CPD)
    for c in range(CPD):
        a = gather_matrix(flat, 2 * CPD, c, mats_a.at[c])
        b = gather_matrix(flat, 2 * CPD, CPD + c, mats_b.at[c])
        sides[c] = a
        sides[CPD + c] = b
        scatter_matrix(dot_tn(a, b), mats_a.at[c], out, CPD, c)
    fold(out, send, CPD)


def backward_kernel(recv, sides_far, send, flat, mats_a, mats_b, out, sides, sem):
    fetch = pltpu.make_async_copy(sides_far, sides, sem)
    fetch.start()
    unfold(recv, flat, CPD)
    fetch.wait()
    for c in range(CPD):
        g = gather_matrix(flat, CPD, c, mats_a.at[c])
        scatter_matrix(dot_nt(sides[CPD + c], g), mats_a.at[c], out, 2 * CPD, c)
        scatter_matrix(dot_nn(sides[c], g), mats_b.at[c], out, 2 * CPD, CPD + c)
    fold(out, send, 2 * CPD)


SMEM = pl.BlockSpec(memory_space=pltpu.SMEM)
HERE = pl.BlockSpec(memory_space=pltpu.VMEM)


def product(kernel, args, out_shape, width_in, width_out, name, in_specs=None, extra=()):
    return pl.pallas_call(
        kernel,
        out_shape=out_shape,
        in_specs=[HERE] if in_specs is None else in_specs,
        scratch_shapes=[
            pltpu.VMEM((LTILES * DEVS * width_in, LANES), F32),
            pltpu.VMEM((CPD, 2 * RES, LANES), F32),
            pltpu.VMEM((CPD, 2 * RES, LANES), F32),
            pltpu.VMEM((LTILES * DEVS * width_out, LANES), F32),
            *extra,
        ],
        name=name,
    )(*args)


def whole(shape):
    return pl.BlockSpec(shape, lambda i: (0,) * len(shape))


def tiled(*lead):
    return pl.BlockSpec((*lead, TILE), lambda i: (0,) * len(lead) + (i,))


ROW_BLOCK = pl.BlockSpec((TROWS, RES, CH), lambda i: (i, 0, 0))
GAIN = whole((1, CH))
LANE_INFO = whole((1, RES))
WIDE_ROW = [pltpu.VMEM((8, 2 * RES), jnp.int32)]
SQUARE = whole((CH, CH))
WIDE = whole((CH, 4 * CH))
COLS = tiled(CH)


def over_tiles(kernel, args, in_specs, out_specs, out_shape, name, scratch=()):
    return pl.pallas_call(
        kernel,
        grid=(STEPS,),
        in_specs=in_specs,
        out_specs=out_specs,
        out_shape=out_shape,
        scratch_shapes=scratch,
        cost_estimate=pl.CostEstimate(flops=1 << 30, bytes_accessed=1 << 22, transcendentals=0),
        name=name,
    )(*args)


def shaped(shape, dtype=BF16):
    return jax.ShapeDtypeStruct(shape, dtype)


def near(shape, dtype=BF16):
    return pltpu.VMEM(shape, dtype)


def exchange(v):
    return pltpu.with_memory_space_constraint(lax.all_to_all(v, AXIS, 0, 0), pltpu.VMEM)


def shards(
    pair,
    cotangent,
    residue_mask,
    chain_ids,
    chain_embed,
    out_norm_gain,
    out_proj,
    out_gate,
    out_mid_gain,
    out_final,
    in_norm_gain,
    in_proj,
    in_gate,
    in_mid_gain,
    in_final,
):
    first = lax.axis_index(AXIS) * (2 * ROWS) + lax.axis_index("cplx") % 2
    first = first.astype(jnp.int32).reshape(1)
    mask_row, chain_row = residue_mask.reshape(1, RES), chain_ids.reshape(1, RES)
    gains = [g.reshape(1, CH) for g in (out_norm_gain, out_mid_gain, in_norm_gain, in_mid_gain)]
    pair_send = near((DEVS, 2 * CPD, POS))
    one_send = near((DEVS, CPD, POS))
    cols = shaped((CH, POS))
    cols_f32 = shaped((CH, POS), F32)

    chains = (first, chain_ids, chain_row, pair, chain_embed, gains[0])
    (send,) = over_tiles(
        first_kernel,
        (first, residue_mask, chain_ids, mask_row, chain_row, pair, chain_embed, gains[0], out_proj),
        [SMEM, SMEM, SMEM, LANE_INFO, LANE_INFO, ROW_BLOCK, whole((2, CH)), GAIN, WIDE],
        [HERE],
        [pair_send],
        "first",
        WIDE_ROW,
    )
    recv = exchange(send)
    start, gated = over_tiles(
        gate_kernel,
        (*chains, out_gate),
        [SMEM, SMEM, LANE_INFO, ROW_BLOCK, whole((2, CH)), GAIN, SQUARE],
        [COLS, COLS],
        [cols_f32, cols_f32],
        "gate",
        WIDE_ROW,
    )
    x_out = product(outgoing_kernel, (first, recv), one_send, 2 * CPD, CPD, "outgoing", [SMEM, HERE])
    send, pair_mid, in_normed = over_tiles(
        middle_kernel,
        (first, residue_mask, mask_row, exchange(x_out), start, gated, gains[1], out_final, gains[2], in_proj),
        [SMEM, SMEM, LANE_INFO, HERE, COLS, COLS, GAIN, SQUARE, GAIN, WIDE],
        [HERE, COLS, COLS],
        [pair_send, cols, cols],
        "middle",
        WIDE_ROW,
    )
    recv = exchange(send)
    grad_value, grad_h, factor, factors = over_tiles(
        ahead_kernel,
        (first, residue_mask, mask_row, cotangent, in_normed, gains[3], in_gate, in_final, in_proj),
        [SMEM, SMEM, LANE_INFO, ROW_BLOCK, COLS, GAIN, SQUARE, SQUARE, WIDE],
        [COLS, COLS, COLS, tiled(4 * CH)],
        [cols, cols, cols_f32, shaped((4 * CH, POS))],
        "ahead",
        WIDE_ROW,
    )
    x_in, sides = product(
        incoming_kernel,
        (recv,),
        [one_send, shaped((2 * CPD, RES, RES))],
        2 * CPD,
        CPD,
        "incoming",
    )
    recv = exchange(x_in)
    send = over_tiles(turn_kernel, (recv, grad_h), [HERE, COLS], HERE, one_send, "turn")
    recv_x = exchange(send)
    sums, from_gate = over_tiles(
        after_kernel,
        (recv, in_normed, grad_value, factor, gains[3], in_final, in_gate),
        [HERE, COLS, COLS, COLS, GAIN, SQUARE, SQUARE],
        [whole((CH, 3 * CH)), COLS],
        [shaped((CH, 3 * CH), F32), cols_f32],
        "after",
    )
    grads = product(backward_kernel, (recv_x, sides), pair_send, CPD, 2 * CPD, "backward",
                    [HERE, pl.BlockSpec(memory_space=pl.ANY)],
                    [pltpu.VMEM((2 * CPD, RES, RES), BF16), pltpu.SemaphoreType.DMA])
    gs = exchange(grads)
    (packed,) = over_tiles(
        last_kernel,
        (gs, in_normed, factors, sums),
        [HERE, COLS, tiled(4 * CH), whole((CH, 3 * CH))],
        [HERE],
        [near((DEVS, CPD, GCOLS))],
        "last",
        [pltpu.VMEM((CH, 4 * CH), F32)],
    )
    parts = exchange(packed)
    pair_grad, gain_rows = over_tiles(
        norm_kernel,
        (cotangent, pair_mid, gs, factors, from_gate, gains[2], in_proj, sums),
        [ROW_BLOCK, COLS, HERE, tiled(4 * CH), COLS, GAIN, WIDE, whole((CH, 3 * CH))],
        [ROW_BLOCK, whole((CPD, CH))],
        [shaped((ROWS, RES, CH)), shaped((CPD, CH), F32)],
        "norm",
        [pltpu.VMEM((CH, LANES), F32)],
    )
    total = pl.pallas_call(
        add_kernel, out_shape=near((DEVS, CPD, GCOLS + CH)), name="add"
    )(parts, gain_rows)
    row = shaped((1, CH), F32)
    grad_proj, grad_gate, grad_final, grad_norm, grad_mid = pl.pallas_call(
        unpack_kernel,
        out_shape=[shaped((CH, 4 * CH), F32), shaped((CH, CH), F32), shaped((CH, CH), F32), row, row],
        name="unpack",
    )(exchange(total))
    return pair_grad, grad_proj, grad_gate, grad_final, grad_norm.reshape(CH), grad_mid.reshape(CH)


def solution(mesh):
    rows = P("dap", "cplx", None)
    return jax.shard_map(
        shards,
        mesh=mesh,
        in_specs=(rows, rows, P("cplx"), P("cplx")) + (P(),) * 11,
        out_specs=(
            rows,
            P("cplx", None),
            P("cplx", None),
            P("cplx", None),
            P("cplx"),
            P("cplx"),
        ),
        check_vma=False,
    )
```
